32 devices in a mesh: rows: 8 (over z, x), cols: 4 (over y, core).
Axes of the slice: x: 2, y: 2, z: 4, core: 2. Of those that a mesh axis runs over, the one named last changes fastest.
Arguments:
- grad_out: bfloat16 [32, 512, 192], P(('rows', 'cols')), may hold values from -6 to 6
- inputs: bfloat16 [64, 1024, 192], P('rows', 'cols'), may hold values from -6 to 6
- weight: bfloat16 [3, 3, 192, 192], replicated, may hold values from -0.15625 to 0.15625
Outputs:
- input_grad: bfloat16 [64, 1024, 192], P('rows', 'cols')
- filter_grad: float32 [3, 3, 192, 192], replicated
The draws below stay inside these ranges and needn't reach their ends.
All inputs are finite; a program needn't handle non-finite values.
Results may differ from the reference program's by a relative error of at most 0.0028.
Values may be sent and summed in bfloat16 or wider, within the bound.
A program may use at most 64 MiB of HBM per device.

```python
import jax
import jax.numpy as jnp
from jax import lax

C = 192
ROWS_DEV = 8
HEIGHT = 64
WIDTH = 1024
POSITIONS = 16384


def steps_of(key, dims, cuts, least, largest):
    def one(dim, parts):
        draws = jax.random.uniform(jax.random.fold_in(jax.random.fold_in(key, 6), dim), (parts,), jnp.float32, least / len(cuts), largest / len(cuts))
        return jnp.repeat(jnp.exp(draws), dims[dim] // parts).reshape((-1,) + (1,) * (len(dims) - dim - 1))

    level = one(*cuts[0])
    for cut in cuts[1:]:
        level = level * one(*cut)
    return level


def bell_draw(rng, extent, scale, most, shards=(), kind=jnp.bfloat16):
    drawn = jax.random.normal(rng, extent, jnp.float32) * scale
    if len(shards) > 0:
        drawn = steps_of(rng, extent, shards, -0.22, 0.18) * drawn
    return jnp.clip(drawn, min=-most, max=most).astype(kind)


def setup_inputs(seed: int = 0) -> dict:
    key_of = jax.random.split(jax.random.key(seed), 4)
    return {
        "grad_out": bell_draw(key_of[0], (HEIGHT // 2, WIDTH // 2, C), 1.0, 6.0, ((0, 32),)),
        "inputs": bell_draw(key_of[1], (HEIGHT, WIDTH, C), 1.0, 6.0, ((0, 8), (1, 4))),
        "weight": bell_draw(key_of[2], (3, 3, C, C), (9 * C) ** -0.5, 0.15625),
    }


def tap_products(out_block, flat_weight):
    chans = flat_weight.shape[0]
    flat = out_block.reshape(-1, chans)
    products = jnp.dot(flat, flat_weight, preferred_element_type=jnp.float32)
    return products.reshape(out_block.shape[0], out_block.shape[1], 3, 3, chans)

def assemble(products, count_rows, count_cols):
    rows_even = products[:count_rows, :, 1]
    rows_odd = products[:count_rows, :, 2] + products[1:count_rows + 1, :, 0]

    def columns(mixed):
        even = mixed[:, :count_cols, 1]
        odd = mixed[:, :count_cols, 2] + mixed[:, 1:count_cols + 1, 0]
        return jnp.stack([even, odd], axis=2)
    placed = jnp.stack([columns(rows_even), columns(rows_odd)], axis=1)
    return placed.reshape(2 * count_rows, 2 * count_cols, products.shape[-1])

def filter_terms(input_band, out_band, row_taps):
    count_rows, count_cols, chans = out_band.shape
    split = input_band.reshape(count_rows + 1, 2, count_cols + 1, 2, chans)
    offsets = ((0, 0), (0, 1), (1, 0))
    pieces = []
    for row_tap in row_taps:
        start_row, parity_row = offsets[row_tap]
        for col_tap in range(3):
            start_col, parity_col = offsets[col_tap]
            pieces.append(split[start_row:start_row + count_rows, parity_row, start_col:start_col + count_cols, parity_col])
    stacked = jnp.stack(pieces, axis=2).reshape(count_rows * count_cols, len(pieces) * chans)
    flat_out = out_band.reshape(count_rows * count_cols, chans)
    return lax.dot_general(stacked, flat_out, (((0,), (0,)), ((), ())), preferred_element_type=jnp.float32)

def reference(grad_out, inputs, weight):
    half_rows, half_cols, chans = grad_out.shape
    band_rows = ROWS_DEV // 2
    flat_weight = jnp.transpose(weight, (3, 0, 1, 2)).reshape(chans, 9 * chans)
    padded_out = jnp.pad(grad_out, ((0, 1), (0, 1), (0, 0)))
    padded_in = jnp.pad(inputs, ((1, 1), (1, 1), (0, 0)))

    def step(total, index):
        start = (index * band_rows).astype(jnp.int32)
        out_block = lax.dynamic_slice_in_dim(padded_out, start, band_rows + 1, 0)
        input_band = lax.dynamic_slice_in_dim(padded_in, (2 * start).astype(jnp.int32), 2 * band_rows + 2, 0)
        block = assemble(tap_products(out_block, flat_weight), band_rows, half_cols).astype(jnp.bfloat16)
        terms = filter_terms(input_band, out_block[:band_rows, :half_cols], (0, 1, 2))
        return (total + terms, block)
    total, blocks = lax.scan(step, jnp.zeros((9 * chans, chans), jnp.float32), jnp.arange(half_rows // band_rows, dtype=jnp.int32))
    input_grad = blocks.reshape(2 * half_rows, 2 * half_cols, chans)
    filter_grad = total.reshape(3, 3, chans, chans) / jnp.sqrt(jnp.float32(POSITIONS))
    return (input_grad, filter_grad)
```

```python
import functools
import math

import jax
import jax.numpy as jnp
from jax import lax
from jax.experimental import pallas as pl
from jax.experimental.pallas import tpu as pltpu
from jax.sharding import PartitionSpec as P

MESH = pl.DeviceIdType.MESH
LANES = 128
EDGE = 16
F32 = jnp.float32
BF16 = jnp.bfloat16
PARITY = (1, 0, 1)
SHIFT = (1, 0, 0)


def spread_matrix(size, transpose):
    half = size // 2
    i = lax.broadcasted_iota(jnp.int32, (size, size), 1 if transpose else 0)
    k = lax.broadcasted_iota(jnp.int32, (size, size), 0 if transpose else 1)
    source = jnp.where(i < half, 2 * i, 2 * (i - half) + 1)
    return jnp.where(k == source, 1.0, 0.0).astype(BF16)


def nt(a, b):
    return lax.dot_general(a, b, (((1,), (1,)), ((), ())), preferred_element_type=F32)


def step_kernel(
    n_rows, n_cols, scale,
    g_ref, x_hbm, w_hbm, ig_ref, sum_ref,
    x, w, gm, gh, gs, xt, part, pair, outbox, inbox, full,
    load_sem, main_s, main_r, halo_s, halo_r, up_s, pair_s, pair_r,
    rs_s, rs_r, ag_s, ag_r, fw_s, fw_r,
):
    r = lax.axis_index("rows")
    c = lax.axis_index("cols")
    core = lax.rem(c, 2)
    depth = n_cols // 2
    chips = n_rows * depth
    chip = r * depth + c // 2
    partner = (r, c + 1 - 2 * core)
    half_rows = n_cols
    half_cols = g_ref.shape[1] // n_cols
    chans = g_ref.shape[2]
    count = outbox.shape[0]
    base = core * count
    devices = n_rows * n_cols
    me = r * n_cols + c

    barrier = pltpu.get_barrier_semaphore()

    def greet(i, _):
        other = lax.rem(me + i, devices)
        pl.semaphore_signal(
            barrier, inc=1, device_id=(other // n_cols, lax.rem(other, n_cols)), device_id_type=MESH
        )
        return 0

    lax.fori_loop(1, devices, greet, 0)
    load_x = pltpu.make_async_copy(x_hbm, x, load_sem.at[0])
    load_w = pltpu.make_async_copy(w_hbm, w, load_sem.at[1])
    load_x.start()
    load_w.start()

    @pl.when(c == n_cols - 1)
    def _():
        gh[...] = jnp.zeros_like(gh)

    @pl.when(r == n_rows - 1)
    def _():
        gm[half_rows] = jnp.zeros(gm.shape[1:], BF16)
        gh[half_rows] = jnp.zeros(gh.shape[1:], BF16)

    for q in range(n_cols):

        @pl.when(c == q)
        def _():
            gm[q] = g_ref[0, q * half_cols : (q + 1) * half_cols]
            if q < n_cols - 1:
                gh[q] = g_ref[0, (q + 1) * half_cols : (q + 1) * half_cols + EDGE]

    pl.semaphore_wait(barrier, devices - 1)

    def main_copy(q, row, slot, send):
        return pltpu.make_async_remote_copy(
            src_ref=g_ref.at[0, pl.ds(q * half_cols, half_cols)], dst_ref=gm.at[slot],
            send_sem=send, recv_sem=main_r.at[slot], device_id=(row, q), device_id_type=MESH,
        )

    def halo_copy(q, row, slot, send):
        return pltpu.make_async_remote_copy(
            src_ref=g_ref.at[0, pl.ds((q + 1) * half_cols, EDGE)], dst_ref=gh.at[slot],
            send_sem=send, recv_sem=halo_r.at[slot], device_id=(row, q), device_id_type=MESH,
        )

    def outgoing(act):
        for q in range(n_cols):

            @pl.when(c != q)
            def _():
                act(main_copy(q, r, c, main_s.at[q]))
                if q < n_cols - 1:
                    act(halo_copy(q, r, c, halo_s.at[q]))

            @pl.when((c == 0) & (r > 0))
            def _():
                act(main_copy(q, r - 1, half_rows, up_s.at[0, q]))
                if q < n_cols - 1:
                    act(halo_copy(q, r - 1, half_rows, up_s.at[1, q]))

    outgoing(lambda copy: copy.start())

    load_x.wait()
    width = x.shape[1]
    sort = spread_matrix(width, False)
    eye = (
        lax.broadcasted_iota(jnp.int32, (chans, chans), 0)
        == lax.broadcasted_iota(jnp.int32, (chans, chans), 1)
    )
    eye = jnp.where(eye, 1.0, 0.0).astype(BF16)
    for p in range(x.shape[0]):
        ordered = jnp.dot(sort, x[p], preferred_element_type=F32).astype(BF16)
        turned = nt(eye, ordered).astype(BF16)
        i = p // 2
        for s in range(2):
            xt[p % 2, s, :, i * half_cols : (i + 1) * half_cols] = turned[
                :, s * half_cols : (s + 1) * half_cols
            ]

    for i in range(half_rows + 1):
        if i < half_rows:
            arrives = c != i
        else:
            arrives = r < n_rows - 1

        @pl.when(arrives)
        def _():
            main_copy(0, r, i, main_s.at[0]).wait_recv()

        @pl.when(arrives & (c < n_cols - 1))
        def _():
            halo_copy(0, r, i, halo_s.at[0]).wait_recv()

        row = jnp.concatenate([gm[i], gh[i]], axis=0).astype(F32)
        gs[i] = row[1 : half_cols + 1].astype(BF16)

    def grad(down, along):
        src = gs if along else gm
        return src[down : down + half_rows].reshape(half_rows * half_cols, chans)

    split = chans // 2
    part[2 * count - 1] = jnp.zeros(part.shape[1:], F32)
    for a in range(3):
        for b in range(3):
            t = 3 * a + b
            terms = jnp.dot(
                xt[PARITY[a], PARITY[b]], grad(SHIFT[a], SHIFT[b]), preferred_element_type=F32
            )
            part[3 * t] = terms[:split, :LANES]
            part[3 * t + 1] = terms[split:, :LANES]
            part[3 * t + 2] = jnp.concatenate([terms[:split, LANES:], terms[split:, LANES:]], axis=1)

    def pair_copy(j):
        return pltpu.make_async_remote_copy(
            src_ref=part.at[(1 - core) * count + j], dst_ref=pair.at[j],
            send_sem=pair_s.at[j], recv_sem=pair_r.at[j], device_id=partner, device_id_type=MESH,
        )

    for j in range(count):
        pair_copy(j).start()

    owners = [(j * chips) // count for j in range(count)]

    def scatter_copy(j):
        return pltpu.make_async_remote_copy(
            src_ref=outbox.at[j], dst_ref=inbox.at[chip],
            send_sem=rs_s.at[j], recv_sem=rs_r.at[chip],
            device_id=(owners[j] // depth, 2 * (owners[j] % depth) + core), device_id_type=MESH,
        )

    for j in range(count):
        pair_copy(j).wait_recv()
        outbox[j] = (part[base + j] + pair[j]).astype(BF16)

        @pl.when(chip != owners[j])
        def _():
            scatter_copy(j).start()

    load_w.wait()
    back = spread_matrix(width, True)

    def tap(a, b):
        return nt(grad(SHIFT[a], SHIFT[b]), w[a, b])

    for odd in range(2):
        taps = (0, 2) if odd else (1,)
        even_cols = sum(tap(a, 1) for a in taps).astype(BF16)
        odd_cols = sum(tap(a, 0) + tap(a, 2) for a in taps).astype(BF16)
        for i in range(half_rows):
            cut = slice(i * half_cols, (i + 1) * half_cols)
            both = jnp.concatenate([even_cols[cut], odd_cols[cut]], axis=0)
            ig_ref[2 * i + odd] = jnp.dot(back, both, preferred_element_type=F32).astype(BF16)

    mine = (chip * count + chips - 1) // chips
    owns = (mine < count) & ((mine * chips) // count == chip)

    def gather_copy(other):
        return pltpu.make_async_remote_copy(
            src_ref=full.at[base + mine], dst_ref=full.at[base + mine],
            send_sem=ag_s.at[other], recv_sem=ag_r.at[mine],
            device_id=(other // depth, 2 * lax.rem(other, depth) + core), device_id_type=MESH,
        )

    @pl.when(owns)
    def _():
        def collect(i, total):
            source = lax.rem(chip + i, chips)
            pltpu.make_async_remote_copy(
                src_ref=outbox.at[0], dst_ref=inbox.at[source],
                send_sem=rs_s.at[0], recv_sem=rs_r.at[source], device_id=partner, device_id_type=MESH,
            ).wait_recv()
            return total + inbox[source].astype(F32)

        total = lax.fori_loop(1, chips, collect, part[base + mine] + pair[mine])
        full[base + mine] = (total * scale).astype(BF16)

        def send(i, _):
            gather_copy(lax.rem(chip + i, chips)).start()
            return 0

        lax.fori_loop(1, chips, send, 0)

    def forward_copy(j, side):
        return pltpu.make_async_remote_copy(
            src_ref=full.at[side * count + j], dst_ref=full.at[side * count + j],
            send_sem=fw_s.at[j], recv_sem=fw_r.at[j], device_id=partner, device_id_type=MESH,
        )

    for j in range(count):

        @pl.when(chip != owners[j])
        def _():
            pltpu.make_async_remote_copy(
                src_ref=outbox.at[0], dst_ref=full.at[base + j],
                send_sem=rs_s.at[0], recv_sem=ag_r.at[j], device_id=partner, device_id_type=MESH,
            ).wait_recv()

        forward_copy(j, core).start()
        sum_ref[base + j] = full[base + j]

    for j in range(count):
        forward_copy(j, 1 - core).wait_recv()
        sum_ref[(1 - core) * count + j] = full[(1 - core) * count + j]

    outgoing(lambda copy: copy.wait_send())
    for j in range(count):
        pair_copy(j).wait_send()
        forward_copy(j, core).wait_send()

        @pl.when(chip != owners[j])
        def _():
            scatter_copy(j).wait_send()

    @pl.when(owns)
    def _():
        def sent(i, _):
            gather_copy(lax.rem(chip + i, chips)).wait_send()
            return 0

        lax.fori_loop(1, chips, sent, 0)


def unpack_kernel(sum_ref, out_ref):
    split = out_ref.shape[1] // 2
    rest = out_ref.shape[2] - LANES
    for t in range(out_ref.shape[0]):
        out_ref[t, :split, :LANES] = sum_ref[3 * t].astype(F32)
        out_ref[t, split:, :LANES] = sum_ref[3 * t + 1].astype(F32)
        packed = sum_ref[3 * t + 2].astype(F32)
        out_ref[t, :split, LANES:] = packed[:, :rest]
        out_ref[t, split:, LANES:] = packed[:, rest:]


def per_device(n_rows, n_cols, grad_out, inputs, weight):
    rows_local, cols_local, chans = inputs.shape
    half_rows, half_cols = rows_local // 2, cols_local // 2
    split = chans // 2
    chips = n_rows * n_cols // 2
    count = (27 + 1) // 2
    scale = 1.0 / math.sqrt(half_rows * n_rows * half_cols * n_cols)
    dma = pltpu.SemaphoreType.DMA
    vmem = pl.BlockSpec(memory_space=pltpu.VMEM)
    anywhere = pl.BlockSpec(memory_space=pl.ANY)
    input_grad, sums = pl.pallas_call(
        functools.partial(step_kernel, n_rows, n_cols, scale),
        out_shape=(
            jax.ShapeDtypeStruct(inputs.shape, BF16),
            jax.ShapeDtypeStruct((2 * count, split, LANES), BF16),
        ),
        in_specs=[vmem, anywhere, anywhere],
        out_specs=(vmem, vmem),
        scratch_shapes=[
            pltpu.VMEM(inputs.shape, BF16),
            pltpu.VMEM(weight.shape, BF16),
            pltpu.VMEM((half_rows + 1, half_cols, chans), BF16),
            pltpu.VMEM((half_rows + 1, EDGE, chans), BF16),
            pltpu.VMEM((half_rows + 1, half_cols, chans), BF16),
            pltpu.VMEM((2, 2, chans, half_rows * half_cols), BF16),
            pltpu.VMEM((2 * count, split, LANES), F32),
            pltpu.VMEM((count, split, LANES), F32),
            pltpu.VMEM((count, split, LANES), BF16),
            pltpu.VMEM((chips, split, LANES), BF16),
            pltpu.VMEM((2 * count, split, LANES), BF16),
            dma((2,)),
            dma((n_cols,)), dma((half_rows + 1,)), dma((n_cols,)), dma((half_rows + 1,)), dma((2, n_cols)),
            dma((count,)), dma((count,)),
            dma((count,)), dma((chips,)), dma((chips,)), dma((count,)),
            dma((count,)), dma((count,)),
        ],
        compiler_params=pltpu.CompilerParams(
            collective_id=0, has_side_effects=True, vmem_limit_bytes=48 * 1024 * 1024
        ),
    )(grad_out, inputs, weight)
    filter_grad = pl.pallas_call(
        unpack_kernel,
        grid=(3,),
        out_shape=jax.ShapeDtypeStruct((9, chans, chans), F32),
        in_specs=[pl.BlockSpec((9, split, LANES), lambda i: (i, 0, 0))],
        out_specs=pl.BlockSpec((3, chans, chans), lambda i: (i, 0, 0)),
    )(sums)
    return input_grad, filter_grad.reshape(3, 3, chans, chans)


def solution(mesh):
    in_specs = (P(("rows", "cols"), None, None), P("rows", "cols", None), P())
    out_specs = (P("rows", "cols", None), P())
    return jax.shard_map(
        functools.partial(per_device, mesh.shape["rows"], mesh.shape["cols"]),
        mesh=mesh, in_specs=in_specs, out_specs=out_specs, check_vma=False,
    )
```

```python
import functools
import math

import jax
import jax.numpy as jnp
from jax import lax
from jax.experimental import pallas as pl
from jax.experimental.pallas import tpu as pltpu
from jax.sharding import PartitionSpec as P

MESH = pl.DeviceIdType.MESH
LANES = 128
EDGE = 16
F32 = jnp.float32
BF16 = jnp.bfloat16
PARITY = (1, 0, 1)
SHIFT = (1, 0, 0)


def iota(shape, dim):
    return lax.broadcasted_iota(jnp.int32, shape, dim)


def ones_where(mask):
    return jnp.where(mask, 1.0, 0.0).astype(BF16)


def spread_matrix(size, back):
    half = size // 2
    i = iota((size, size), 0 if back else 1)
    k = iota((size, size), 1 if back else 0)
    return ones_where(k == jnp.where(i < half, 2 * i, 2 * (i - half) + 1))


def nn(a, b):
    return jnp.dot(a, b, preferred_element_type=F32)


def nt(a, b):
    return lax.dot_general(a, b, (((1,), (1,)), ((), ())), preferred_element_type=F32)


def step_kernel(
    n_rows, n_cols, scale,
    g_ref, x_hbm, w_hbm, ig_ref, sum_ref,
    x, w, gm, gh, gs, edge, xt, part, pair, outbox, inbox, full,
    load_sem, main_s, main_r, halo_s, halo_r, up_s, pair_s, pair_r,
    rs_s, rs_r, ag_s, ag_r, fw_s, fw_r,
):
    r = lax.axis_index("rows")
    c = lax.axis_index("cols")
    core = lax.rem(c, 2)
    depth = n_cols // 2
    chips = n_rows * depth
    chip = r * depth + c // 2
    partner = (r, c + 1 - 2 * core)
    half_rows = n_cols
    half_cols = g_ref.shape[2] // n_cols
    chans = g_ref.shape[1]
    count = outbox.shape[0]
    base = core * count
    devices = n_rows * n_cols
    me = r * n_cols + c

    barrier = pltpu.get_barrier_semaphore()

    def greet(i, _):
        other = lax.rem(me + i, devices)
        pl.semaphore_signal(
            barrier, inc=1, device_id=(other // n_cols, lax.rem(other, n_cols)), device_id_type=MESH
        )
        return 0

    lax.fori_loop(1, devices, greet, 0)
    load_x = pltpu.make_async_copy(x_hbm, x, load_sem.at[0])
    load_w = pltpu.make_async_copy(w_hbm, w, load_sem.at[1])
    load_x.start()
    load_w.start()

    def block(i):
        return slice(i * half_cols, (i + 1) * half_cols)

    @pl.when(r == n_rows - 1)
    def _():
        gm[:, block(half_rows)] = jnp.zeros((chans, half_cols), BF16)
        gh[half_rows] = jnp.zeros(gh.shape[1:], BF16)

    for q in range(n_cols):

        @pl.when(c == q)
        def _():
            gm[:, block(q)] = g_ref[0, :, block(q)]

    full_cols = g_ref.shape[2]
    wanted = (iota((EDGE, full_cols), 0) + 1) * half_cols
    edge[...] = nt(ones_where(wanted == iota((EDGE, full_cols), 1)), g_ref[0]).astype(BF16)
    gh[c] = edge[...]

    pl.semaphore_wait(barrier, devices - 1)

    def main_copy(q, row, slot, send):
        return pltpu.make_async_remote_copy(
            src_ref=g_ref.at[0, :, pl.ds(q * half_cols, half_cols)],
            dst_ref=gm.at[:, pl.ds(pl.multiple_of(slot * half_cols, LANES), half_cols)],
            send_sem=send, recv_sem=main_r.at[slot], device_id=(row, q), device_id_type=MESH,
        )

    def halo_copy(q, row, slot, send):
        return pltpu.make_async_remote_copy(
            src_ref=edge, dst_ref=gh.at[slot],
            send_sem=send, recv_sem=halo_r.at[slot], device_id=(row, q), device_id_type=MESH,
        )

    def outgoing(act):
        for q in range(n_cols):

            @pl.when((c == 0) & (r > 0))
            def _():
                act(main_copy(q, r - 1, half_rows, up_s.at[0, q]))
                act(halo_copy(q, r - 1, half_rows, up_s.at[1, q]))

            @pl.when(c != q)
            def _():
                act(main_copy(q, r, c, main_s.at[q]))
                act(halo_copy(q, r, c, halo_s.at[q]))

    outgoing(lambda copy: copy.start())

    load_x.wait()
    width = x.shape[2]
    sort = spread_matrix(width, False)
    for p in range(x.shape[0]):
        ordered = nn(x[p], sort).astype(BF16)
        for s in range(2):
            xt[p % 2, s, :, block(p // 2)] = ordered[:, block(s)]

    for i in range(half_rows + 1):
        if i < half_rows:
            arrives = c != i
        else:
            arrives = r < n_rows - 1

        @pl.when(arrives)
        def _():
            main_copy(0, r, i, main_s.at[0]).wait_recv()
            halo_copy(0, r, i, halo_s.at[0]).wait_recv()

    slots = half_rows + 1
    eye = ones_where(iota((chans, chans), 0) == iota((chans, chans), 1))
    turned = nt(eye, gh[...].reshape(slots * EDGE, chans)).astype(BF16)
    shift = ones_where(iota((half_cols, half_cols), 0) == iota((half_cols, half_cols), 1) + 1)
    for i in range(slots):
        place = (slots * EDGE, half_cols)
        last = (iota(place, 0) == i * EDGE + c) & (iota(place, 1) == half_cols - 1)
        gs[:, block(i)] = (nn(gm[:, block(i)], shift) + nn(turned, ones_where(last))).astype(BF16)

    def grad(down, along):
        src = gs if along else gm
        return src[:, down * half_cols : (down + half_rows) * half_cols]

    split = chans // 2
    part[2 * count - 1] = jnp.zeros(part.shape[1:], F32)
    for a in range(3):
        for b in range(3):
            t = 3 * a + b
            terms = nt(xt[PARITY[a], PARITY[b]], grad(SHIFT[a], SHIFT[b]))
            part[3 * t] = terms[:split, :LANES]
            part[3 * t + 1] = terms[split:, :LANES]
            part[3 * t + 2] = jnp.concatenate([terms[:split, LANES:], terms[split:, LANES:]], axis=1)

    def pair_copy(j):
        return pltpu.make_async_remote_copy(
            src_ref=part.at[(1 - core) * count + j], dst_ref=pair.at[j],
            send_sem=pair_s.at[j], recv_sem=pair_r.at[j], device_id=partner, device_id_type=MESH,
        )

    upper = chip // (chips // 2)
    half_count = count // 2

    def far_first(i):
        near = i // half_count
        side = upper * near + (1 - upper) * (1 - near)
        return side * half_count + lax.rem(chip + i, half_count)

    def owner_of(j):
        return (j * chips) // count

    for i in range(count):
        pair_copy(far_first(i)).start()

    def scatter_copy(j):
        owner = owner_of(j)
        return pltpu.make_async_remote_copy(
            src_ref=outbox.at[j], dst_ref=inbox.at[chip],
            send_sem=rs_s.at[j], recv_sem=rs_r.at[chip],
            device_id=(owner // depth, 2 * lax.rem(owner, depth) + core), device_id_type=MESH,
        )

    for i in range(count):
        j = far_first(i)
        pair_copy(j).wait_recv()
        outbox[j] = (part[base + j] + pair[j]).astype(BF16)

        @pl.when(chip != owner_of(j))
        def _():
            scatter_copy(j).start()

    load_w.wait()
    back = spread_matrix(width, True)

    def tap(a, b):
        return nn(w[a, b], grad(SHIFT[a], SHIFT[b]))

    for odd in range(2):
        taps = (0, 2) if odd else (1,)
        even_cols = sum(tap(a, 1) for a in taps).astype(BF16)
        odd_cols = sum(tap(a, 0) + tap(a, 2) for a in taps).astype(BF16)
        for i in range(half_rows):
            both = jnp.concatenate([even_cols[:, block(i)], odd_cols[:, block(i)]], axis=1)
            ig_ref[2 * i + odd] = nn(both, back).astype(BF16)

    mine = (chip * count + chips - 1) // chips
    owns = (mine < count) & ((mine * chips) // count == chip)

    def gather_copy(other):
        return pltpu.make_async_remote_copy(
            src_ref=full.at[base + mine], dst_ref=full.at[base + mine],
            send_sem=ag_s.at[other], recv_sem=ag_r.at[mine],
            device_id=(other // depth, 2 * lax.rem(other, depth) + core), device_id_type=MESH,
        )

    @pl.when(owns)
    def _():
        def collect(i, total):
            source = lax.rem(chip + i, chips)
            pltpu.make_async_remote_copy(
                src_ref=outbox.at[0], dst_ref=inbox.at[source],
                send_sem=rs_s.at[0], recv_sem=rs_r.at[source], device_id=partner, device_id_type=MESH,
            ).wait_recv()
            return total + inbox[source].astype(F32)

        total = lax.fori_loop(1, chips, collect, part[base + mine] + pair[mine])
        full[base + mine] = (total * scale).astype(BF16)

        def send(i, _):
            near = i // (chips // 2)
            side = upper * near + (1 - upper) * (1 - near)
            other = side * (chips // 2) + lax.rem(chip + i, chips // 2)

            @pl.when(other != chip)
            def _():
                gather_copy(other).start()

            return 0

        lax.fori_loop(0, chips, send, 0)

    def forward_copy(j, side):
        return pltpu.make_async_remote_copy(
            src_ref=full.at[side * count + j], dst_ref=full.at[side * count + j],
            send_sem=fw_s.at[j], recv_sem=fw_r.at[j], device_id=partner, device_id_type=MESH,
        )

    for j in range(count):

        @pl.when(chip != owner_of(j))
        def _():
            pltpu.make_async_remote_copy(
                src_ref=outbox.at[0], dst_ref=full.at[base + j],
                send_sem=rs_s.at[0], recv_sem=ag_r.at[j], device_id=partner, device_id_type=MESH,
            ).wait_recv()

        forward_copy(j, core).start()
        sum_ref[base + j] = full[base + j]

    for j in range(count):
        forward_copy(j, 1 - core).wait_recv()
        sum_ref[(1 - core) * count + j] = full[(1 - core) * count + j]

    outgoing(lambda copy: copy.wait_send())
    for j in range(count):
        pair_copy(j).wait_send()
        forward_copy(j, core).wait_send()

        @pl.when(chip != owner_of(j))
        def _():
            scatter_copy(j).wait_send()

    @pl.when(owns)
    def _():
        def sent(i, _):
            gather_copy(lax.rem(chip + i, chips)).wait_send()
            return 0

        lax.fori_loop(1, chips, sent, 0)


def unpack_kernel(ig_ref, sum_ref, ig_out, filter_out, wide, sems):
    split = wide.shape[1] // 2
    rest = wide.shape[2] - LANES
    taps = wide.shape[0]
    whole = pltpu.make_async_copy(ig_ref, ig_out, sems.at[taps])
    whole.start()
    copies = []
    for t in range(taps):
        wide[t, :split, :LANES] = sum_ref[3 * t].astype(F32)
        wide[t, split:, :LANES] = sum_ref[3 * t + 1].astype(F32)
        packed = sum_ref[3 * t + 2].astype(F32)
        wide[t, :split, LANES:] = packed[:, :rest]
        wide[t, split:, LANES:] = packed[:, rest:]
        copies.append(pltpu.make_async_copy(wide.at[t], filter_out.at[t], sems.at[t]))
        copies[-1].start()
    whole.wait()
    for copy in copies:
        copy.wait()


def per_device(n_rows, n_cols, grad_out, inputs, weight):
    rows_local, cols_local, chans = inputs.shape
    grad_out, inputs = (jnp.swapaxes(grad_out, 1, 2), jnp.swapaxes(inputs, 1, 2))
    half_rows, half_cols = rows_local // 2, cols_local // 2
    split = chans // 2
    chips = n_rows * n_cols // 2
    count = (27 + 1) // 2
    scale = 1.0 / math.sqrt(half_rows * n_rows * half_cols * n_cols)
    dma = pltpu.SemaphoreType.DMA
    vmem = pl.BlockSpec(memory_space=pltpu.VMEM)
    anywhere = pl.BlockSpec(memory_space=pl.ANY)
    hbm = pl.BlockSpec(memory_space=pltpu.HBM)
    input_grad, sums = pl.pallas_call(
        functools.partial(step_kernel, n_rows, n_cols, scale),
        out_shape=(
            jax.ShapeDtypeStruct(inputs.shape, BF16),
            jax.ShapeDtypeStruct((2 * count, split, LANES), BF16),
        ),
        in_specs=[vmem, hbm, hbm],
        out_specs=(vmem, vmem),
        scratch_shapes=[
            pltpu.VMEM(inputs.shape, BF16),
            pltpu.VMEM(weight.shape, BF16),
            pltpu.VMEM((chans, (half_rows + 1) * half_cols), BF16),
            pltpu.VMEM((half_rows + 1, EDGE, chans), BF16),
            pltpu.VMEM((chans, (half_rows + 1) * half_cols), BF16),
            pltpu.VMEM((EDGE, chans), BF16),
            pltpu.VMEM((2, 2, chans, half_rows * half_cols), BF16),
            pltpu.VMEM((2 * count, split, LANES), F32),
            pltpu.VMEM((count, split, LANES), F32),
            pltpu.VMEM((count, split, LANES), BF16),
            pltpu.VMEM((chips, split, LANES), BF16),
            pltpu.VMEM((2 * count, split, LANES), BF16),
            dma((2,)),
            dma((n_cols,)), dma((half_rows + 1,)), dma((n_cols,)), dma((half_rows + 1,)), dma((2, n_cols)),
            dma((count,)), dma((count,)),
            dma((count,)), dma((chips,)), dma((chips,)), dma((count,)),
            dma((count,)), dma((count,)),
        ],
        compiler_params=pltpu.CompilerParams(
            collective_id=0, has_side_effects=True, vmem_limit_bytes=48 * 1024 * 1024
        ),
    )(grad_out, inputs, weight)
    input_grad, filter_grad = pl.pallas_call(
        unpack_kernel,
        out_shape=(
            jax.ShapeDtypeStruct(inputs.shape, BF16),
            jax.ShapeDtypeStruct((9, chans, chans), F32),
        ),
        in_specs=[vmem, vmem],
        out_specs=(anywhere, anywhere),
        scratch_shapes=[pltpu.VMEM((9, chans, chans), F32), dma((10,))],
        compiler_params=pltpu.CompilerParams(vmem_limit_bytes=12 * 1024 * 1024),
    )(input_grad, sums)
    return jnp.swapaxes(input_grad, 1, 2), filter_grad.reshape(3, 3, chans, chans)


def solution(mesh):
    in_specs = (P(("rows", "cols"), None, None), P("rows", "cols", None), P())
    out_specs = (P("rows", "cols", None), P())
    return jax.shard_map(
        functools.partial(per_device, mesh.shape["rows"], mesh.shape["cols"]),
        mesh=mesh, in_specs=in_specs, out_specs=out_specs, check_vma=False,
    )
```

```python
import functools
import math

import jax
import jax.numpy as jnp
from jax import lax
from jax.experimental import pallas as pl
from jax.experimental.pallas import tpu as pltpu
from jax.sharding import PartitionSpec as P

MESH = pl.DeviceIdType.MESH
LANES = 128
EDGE = 16
F32 = jnp.float32
BF16 = jnp.bfloat16
PARITY = (1, 0, 1)
SHIFT = (1, 0, 0)


def iota(shape, dim):
    return lax.broadcasted_iota(jnp.int32, shape, dim)


def ones_where(mask):
    return jnp.where(mask, 1.0, 0.0).astype(BF16)


def spread_matrix(size, back):
    half = size // 2
    i = iota((size, size), 0 if back else 1)
    k = iota((size, size), 1 if back else 0)
    return ones_where(k == jnp.where(i < half, 2 * i, 2 * (i - half) + 1))


def nn(a, b):
    return jnp.dot(a, b, preferred_element_type=F32)


def nt(a, b):
    return lax.dot_general(a, b, (((1,), (1,)), ((), ())), preferred_element_type=F32)


def step_kernel(
    n_rows, n_cols, scale,
    g_ref, x_hbm, w_hbm, ig_ref, sum_ref,
    x, w, gm, gh, gs, edge, xt, part, pair, outbox, inbox, full,
    load_sem, main_s, main_r, halo_s, halo_r, up_s, pair_s, pair_r,
    rs_s, rs_r, ag_s, ag_r, plane_s, fw_s, fw_r,
):
    r = lax.axis_index("rows")
    c = lax.axis_index("cols")
    core = lax.rem(c, 2)
    depth = n_cols // 2
    chips = n_rows * depth
    chip = r * depth + c // 2
    partner = (r, c + 1 - 2 * core)
    half_rows = n_cols
    half_cols = g_ref.shape[2] // n_cols
    chans = g_ref.shape[1]
    count = outbox.shape[0]
    base = core * count
    devices = n_rows * n_cols
    me = r * n_cols + c

    barrier = pltpu.get_barrier_semaphore()

    def greet(i, _):
        other = lax.rem(me + i, devices)
        pl.semaphore_signal(
            barrier, inc=1, device_id=(other // n_cols, lax.rem(other, n_cols)), device_id_type=MESH
        )
        return 0

    lax.fori_loop(1, devices, greet, 0)
    load_x = pltpu.make_async_copy(x_hbm, x, load_sem.at[0])
    load_w = pltpu.make_async_copy(w_hbm, w, load_sem.at[1])
    load_x.start()
    load_w.start()

    def block(i):
        return slice(i * half_cols, (i + 1) * half_cols)

    @pl.when(r == n_rows - 1)
    def _():
        gm[:, block(half_rows)] = jnp.zeros((chans, half_cols), BF16)
        gh[half_rows] = jnp.zeros(gh.shape[1:], BF16)

    for q in range(n_cols):

        @pl.when(c == q)
        def _():
            gm[:, block(q)] = g_ref[0, :, block(q)]

    full_cols = g_ref.shape[2]
    wanted = (iota((EDGE, full_cols), 0) + 1) * half_cols
    edge[...] = nt(ones_where(wanted == iota((EDGE, full_cols), 1)), g_ref[0]).astype(BF16)
    gh[c] = edge[...]

    pl.semaphore_wait(barrier, devices - 1)

    def main_copy(q, row, slot, send):
        return pltpu.make_async_remote_copy(
            src_ref=g_ref.at[0, :, pl.ds(q * half_cols, half_cols)],
            dst_ref=gm.at[:, pl.ds(pl.multiple_of(slot * half_cols, LANES), half_cols)],
            send_sem=send, recv_sem=main_r.at[slot], device_id=(row, q), device_id_type=MESH,
        )

    def halo_copy(q, row, slot, send):
        return pltpu.make_async_remote_copy(
            src_ref=edge, dst_ref=gh.at[slot],
            send_sem=send, recv_sem=halo_r.at[slot], device_id=(row, q), device_id_type=MESH,
        )

    def outgoing(act):
        for q in range(n_cols):

            @pl.when((c == 0) & (r > 0))
            def _():
                act(main_copy(q, r - 1, half_rows, up_s.at[0, q]))
                act(halo_copy(q, r - 1, half_rows, up_s.at[1, q]))

            @pl.when(c != q)
            def _():
                act(main_copy(q, r, c, main_s.at[q]))
                act(halo_copy(q, r, c, halo_s.at[q]))

    outgoing(lambda copy: copy.start())

    load_x.wait()
    width = x.shape[2]
    sort = spread_matrix(width, False)
    for p in range(x.shape[0]):
        ordered = nn(x[p], sort).astype(BF16)
        for s in range(2):
            xt[p % 2, s, :, block(p // 2)] = ordered[:, block(s)]

    for i in range(half_rows + 1):
        if i < half_rows:
            arrives = c != i
        else:
            arrives = r < n_rows - 1

        @pl.when(arrives)
        def _():
            main_copy(0, r, i, main_s.at[0]).wait_recv()
            halo_copy(0, r, i, halo_s.at[0]).wait_recv()

    slots = half_rows + 1
    eye = ones_where(iota((chans, chans), 0) == iota((chans, chans), 1))
    turned = nt(eye, gh[...].reshape(slots * EDGE, chans)).astype(BF16)
    shift = ones_where(iota((half_cols, half_cols), 0) == iota((half_cols, half_cols), 1) + 1)
    for i in range(slots):
        place = (slots * EDGE, half_cols)
        last = (iota(place, 0) == i * EDGE + c) & (iota(place, 1) == half_cols - 1)
        gs[:, block(i)] = (nn(gm[:, block(i)], shift) + nn(turned, ones_where(last))).astype(BF16)

    def grad(down, along):
        src = gs if along else gm
        return src[:, down * half_cols : (down + half_rows) * half_cols]

    split = chans // 2
    part[2 * count - 1] = jnp.zeros(part.shape[1:], F32)
    for a in range(3):
        for b in range(3):
            t = 3 * a + b
            terms = nt(xt[PARITY[a], PARITY[b]], grad(SHIFT[a], SHIFT[b]))
            part[3 * t] = terms[:split, :LANES]
            part[3 * t + 1] = terms[split:, :LANES]
            part[3 * t + 2] = jnp.concatenate([terms[:split, LANES:], terms[split:, LANES:]], axis=1)

    def pair_copy(j):
        return pltpu.make_async_remote_copy(
            src_ref=part.at[(1 - core) * count + j], dst_ref=pair.at[j],
            send_sem=pair_s.at[j], recv_sem=pair_r.at[j], device_id=partner, device_id_type=MESH,
        )

    upper = chip // (chips // 2)
    half_count = count // 2

    def far_first(i):
        near = i // half_count
        side = upper * near + (1 - upper) * (1 - near)
        return side * half_count + lax.rem(chip + i, half_count)

    def owner_of(j):
        return (j * chips) // count

    for i in range(count):
        pair_copy(far_first(i)).start()

    def scatter_copy(j):
        owner = owner_of(j)
        return pltpu.make_async_remote_copy(
            src_ref=outbox.at[j], dst_ref=inbox.at[chip],
            send_sem=rs_s.at[j], recv_sem=rs_r.at[chip],
            device_id=(owner // depth, 2 * lax.rem(owner, depth) + core), device_id_type=MESH,
        )

    for i in range(count):
        j = far_first(i)
        pair_copy(j).wait_recv()
        outbox[j] = (part[base + j] + pair[j]).astype(BF16)

        @pl.when(chip != owner_of(j))
        def _():
            scatter_copy(j).start()

    load_w.wait()
    back = spread_matrix(width, True)

    def tap(a, b):
        return nn(w[a, b], grad(SHIFT[a], SHIFT[b]))

    for odd in range(2):
        taps = (0, 2) if odd else (1,)
        even_cols = sum(tap(a, 1) for a in taps).astype(BF16)
        odd_cols = sum(tap(a, 0) + tap(a, 2) for a in taps).astype(BF16)
        for i in range(half_rows):
            both = jnp.concatenate([even_cols[:, block(i)], odd_cols[:, block(i)]], axis=1)
            ig_ref[2 * i + odd] = nn(both, back).astype(BF16)

    plane = 2 * depth
    layers = chips // plane
    layer, spot = chip // plane, lax.rem(chip, plane)

    def chunk_of(other):
        return (other * count + chips - 1) // chips

    def owns(other):
        return (chunk_of(other) < count) & (owner_of(chunk_of(other)) == other)

    mine = chunk_of(chip)

    def share(j, row, col, send):
        return pltpu.make_async_remote_copy(
            src_ref=full.at[base + j], dst_ref=full.at[base + j],
            send_sem=send, recv_sem=ag_r.at[j], device_id=(row, col), device_id_type=MESH,
        )

    def to_layers(act):
        @pl.when(owns(chip))
        def _():
            for i in range(layers):
                other = lax.rem(layer + i + layers // 2, layers)

                @pl.when(other != layer)
                def _():
                    act(share(mine, 2 * other + spot // depth, c, ag_s.at[other]))

    def to_plane(source_layer, act):
        j = chunk_of(source_layer * plane + spot)
        for i in range(1, plane):
            other = lax.rem(spot + i, plane)
            act(share(
                j, 2 * layer + other // depth, 2 * lax.rem(other, depth) + core,
                plane_s.at[source_layer, other],
            ))

    def forward_copy(j, side):
        return pltpu.make_async_remote_copy(
            src_ref=full.at[side * count + j], dst_ref=full.at[side * count + j],
            send_sem=fw_s.at[j], recv_sem=fw_r.at[j], device_id=partner, device_id_type=MESH,
        )

    def pass_on(j):
        forward_copy(j, core).start()
        sum_ref[base + j] = full[base + j]

    @pl.when(owns(chip))
    def _():
        def collect(i, total):
            source = lax.rem(chip + i, chips)
            pltpu.make_async_remote_copy(
                src_ref=outbox.at[0], dst_ref=inbox.at[source],
                send_sem=rs_s.at[0], recv_sem=rs_r.at[source], device_id=partner, device_id_type=MESH,
            ).wait_recv()
            return total + inbox[source].astype(F32)

        total = lax.fori_loop(1, chips, collect, part[base + mine] + pair[mine])
        full[base + mine] = (total * scale).astype(BF16)

    to_layers(lambda copy: copy.start())

    @pl.when(owns(chip))
    def _():
        to_plane(layer, lambda copy: copy.start())
        pass_on(mine)

    def relay(i, _):
        source_layer = lax.rem(layer + i, layers)
        source = source_layer * plane + spot

        @pl.when(owns(source))
        def _():
            share(chunk_of(source), r, c, ag_s.at[layer]).wait_recv()
            to_plane(source_layer, lambda copy: copy.start())
            pass_on(chunk_of(source))

        return 0

    lax.fori_loop(1, layers, relay, 0)

    def take(i, _):
        source = lax.rem(layer + i // (plane - 1), layers) * plane + lax.rem(
            spot + 1 + lax.rem(i, plane - 1), plane
        )

        @pl.when(owns(source))
        def _():
            share(chunk_of(source), r, c, ag_s.at[layer]).wait_recv()
            pass_on(chunk_of(source))

        return 0

    lax.fori_loop(0, layers * (plane - 1), take, 0)

    for j in range(count):
        forward_copy(j, 1 - core).wait_recv()
        sum_ref[(1 - core) * count + j] = full[(1 - core) * count + j]

    outgoing(lambda copy: copy.wait_send())
    for j in range(count):
        pair_copy(j).wait_send()
        forward_copy(j, core).wait_send()

        @pl.when(chip != owner_of(j))
        def _():
            scatter_copy(j).wait_send()

    to_layers(lambda copy: copy.wait_send())

    def sent(i, _):
        @pl.when(owns(i * plane + spot))
        def _():
            to_plane(i, lambda copy: copy.wait_send())

        return 0

    lax.fori_loop(0, layers, sent, 0)


def unpack_kernel(ig_ref, sum_ref, ig_out, filter_out, wide, sems):
    split = wide.shape[1] // 2
    rest = wide.shape[2] - LANES
    taps = wide.shape[0]
    whole = pltpu.make_async_copy(ig_ref, ig_out, sems.at[taps])
    whole.start()
    copies = []
    for t in range(taps):
        wide[t, :split, :LANES] = sum_ref[3 * t].astype(F32)
        wide[t, split:, :LANES] = sum_ref[3 * t + 1].astype(F32)
        packed = sum_ref[3 * t + 2].astype(F32)
        wide[t, :split, LANES:] = packed[:, :rest]
        wide[t, split:, LANES:] = packed[:, rest:]
        copies.append(pltpu.make_async_copy(wide.at[t], filter_out.at[t], sems.at[t]))
        copies[-1].start()
    whole.wait()
    for copy in copies:
        copy.wait()


def per_device(n_rows, n_cols, grad_out, inputs, weight):
    rows_local, cols_local, chans = inputs.shape
    grad_out, inputs = (jnp.swapaxes(grad_out, 1, 2), jnp.swapaxes(inputs, 1, 2))
    inputs = pltpu.with_memory_space_constraint(inputs, pltpu.HBM)
    weight = pltpu.with_memory_space_constraint(weight, pltpu.HBM)
    half_rows, half_cols = rows_local // 2, cols_local // 2
    split = chans // 2
    chips = n_rows * n_cols // 2
    count = (27 + 1) // 2
    scale = 1.0 / math.sqrt(half_rows * n_rows * half_cols * n_cols)
    dma = pltpu.SemaphoreType.DMA
    vmem = pl.BlockSpec(memory_space=pltpu.VMEM)
    anywhere = pl.BlockSpec(memory_space=pl.ANY)
    hbm = pl.BlockSpec(memory_space=pltpu.HBM)
    input_grad, sums = pl.pallas_call(
        functools.partial(step_kernel, n_rows, n_cols, scale),
        out_shape=(
            jax.ShapeDtypeStruct(inputs.shape, BF16),
            jax.ShapeDtypeStruct((2 * count, split, LANES), BF16),
        ),
        in_specs=[vmem, hbm, hbm],
        out_specs=(vmem, vmem),
        scratch_shapes=[
            pltpu.VMEM(inputs.shape, BF16),
            pltpu.VMEM(weight.shape, BF16),
            pltpu.VMEM((chans, (half_rows + 1) * half_cols), BF16),
            pltpu.VMEM((half_rows + 1, EDGE, chans), BF16),
            pltpu.VMEM((chans, (half_rows + 1) * half_cols), BF16),
            pltpu.VMEM((EDGE, chans), BF16),
            pltpu.VMEM((2, 2, chans, half_rows * half_cols), BF16),
            pltpu.VMEM((2 * count, split, LANES), F32),
            pltpu.VMEM((count, split, LANES), F32),
            pltpu.VMEM((count, split, LANES), BF16),
            pltpu.VMEM((chips, split, LANES), BF16),
            pltpu.VMEM((2 * count, split, LANES), BF16),
            dma((2,)),
            dma((n_cols,)), dma((half_rows + 1,)), dma((n_cols,)), dma((half_rows + 1,)), dma((2, n_cols)),
            dma((count,)), dma((count,)),
            dma((count,)), dma((chips,)), dma((chips,)), dma((count,)), dma((chips // n_cols, n_cols)),
            dma((count,)), dma((count,)),
        ],
        compiler_params=pltpu.CompilerParams(
            collective_id=0, has_side_effects=True, vmem_limit_bytes=48 * 1024 * 1024
        ),
    )(grad_out, inputs, weight)
    input_grad, filter_grad = pl.pallas_call(
        unpack_kernel,
        out_shape=(
            jax.ShapeDtypeStruct(inputs.shape, BF16),
            jax.ShapeDtypeStruct((9, chans, chans), F32),
        ),
        in_specs=[vmem, vmem],
        out_specs=(anywhere, anywhere),
        scratch_shapes=[pltpu.VMEM((9, chans, chans), F32), dma((10,))],
        compiler_params=pltpu.CompilerParams(vmem_limit_bytes=12 * 1024 * 1024),
    )(input_grad, sums)
    return jnp.swapaxes(input_grad, 1, 2), filter_grad.reshape(3, 3, chans, chans)


def solution(mesh):
    in_specs = (P(("rows", "cols"), None, None), P("rows", "cols", None), P())
    out_specs = (P("rows", "cols", None), P())
    return jax.shard_map(
        functools.partial(per_device, mesh.shape["rows"], mesh.shape["cols"]),
        mesh=mesh, in_specs=in_specs, out_specs=out_specs, check_vma=False,
    )
```

```python
import functools
import math

import jax
import jax.numpy as jnp
from jax import lax
from jax.experimental import pallas as pl
from jax.experimental.pallas import tpu as pltpu
from jax.sharding import PartitionSpec as P

MESH = pl.DeviceIdType.MESH
LANES = 128
EDGE = 16
PIECES = 2
F32 = jnp.float32
BF16 = jnp.bfloat16
PARITY = (1, 0, 1)
SHIFT = (1, 0, 0)


def iota(shape, dim):
    return lax.broadcasted_iota(jnp.int32, shape, dim)


def ones_where(mask):
    return jnp.where(mask, 1.0, 0.0).astype(BF16)


def spread_matrix(size, back):
    half = size // 2
    i = iota((size, size), 0 if back else 1)
    k = iota((size, size), 1 if back else 0)
    return ones_where(k == jnp.where(i < half, 2 * i, 2 * (i - half) + 1))


def nn(a, b):
    return jnp.dot(a, b, preferred_element_type=F32)


def nt(a, b):
    return lax.dot_general(a, b, (((1,), (1,)), ((), ())), preferred_element_type=F32)


def step_kernel(
    n_rows, n_cols, scale,
    g_hbm, x_hbm, w_hbm, ig_ref, sum_ref,
    g_ref, x, w, gm, gh, gs, edge, xt, part, pair, outbox, inbox, full,
    load_sem, main_s, main_r, halo_s, halo_r, up_s, pair_s, pair_r,
    rs_s, rs_r, ag_s, ag_r, plane_s, fw_s, fw_r,
):
    r = lax.axis_index("rows")
    c = lax.axis_index("cols")
    core = lax.rem(c, 2)
    depth = n_cols // 2
    chips = n_rows * depth
    chip = r * depth + c // 2
    partner = (r, c + 1 - 2 * core)
    half_rows = n_cols
    half_cols = g_ref.shape[2] // n_cols
    chans = g_ref.shape[1]
    count = outbox.shape[0]
    base = core * count
    devices = n_rows * n_cols
    me = r * n_cols + c

    barrier = pltpu.get_barrier_semaphore()

    def greet(i, _):
        other = lax.rem(me + i, devices)
        pl.semaphore_signal(
            barrier, inc=1, device_id=(other // n_cols, lax.rem(other, n_cols)), device_id_type=MESH
        )
        return 0

    lax.fori_loop(1, devices, greet, 0)
    load_x = pltpu.make_async_copy(x_hbm, x, load_sem.at[0])
    load_w = pltpu.make_async_copy(w_hbm, w, load_sem.at[1])
    load_g = pltpu.make_async_copy(g_hbm, g_ref, load_sem.at[2])
    load_g.start()
    load_x.start()
    load_w.start()

    def block(i):
        return slice(i * half_cols, (i + 1) * half_cols)

    @pl.when(r == n_rows - 1)
    def _():
        gm[:, block(half_rows)] = jnp.zeros((chans, half_cols), BF16)
        gh[half_rows] = jnp.zeros(gh.shape[1:], BF16)

    load_g.wait()
    for q in range(n_cols):

        @pl.when(c == q)
        def _():
            gm[:, block(q)] = g_ref[0, :, block(q)]

    full_cols = g_ref.shape[2]
    wanted = (iota((EDGE, full_cols), 0) + 1) * half_cols
    edge[...] = nt(ones_where(wanted == iota((EDGE, full_cols), 1)), g_ref[0]).astype(BF16)
    gh[c] = edge[...]

    pl.semaphore_wait(barrier, devices - 1)

    def main_copy(q, row, slot, send):
        return pltpu.make_async_remote_copy(
            src_ref=g_ref.at[0, :, pl.ds(q * half_cols, half_cols)],
            dst_ref=gm.at[:, pl.ds(pl.multiple_of(slot * half_cols, LANES), half_cols)],
            send_sem=send, recv_sem=main_r.at[slot], device_id=(row, q), device_id_type=MESH,
        )

    def halo_copy(q, row, slot, send):
        return pltpu.make_async_remote_copy(
            src_ref=edge, dst_ref=gh.at[slot],
            send_sem=send, recv_sem=halo_r.at[slot], device_id=(row, q), device_id_type=MESH,
        )

    def outgoing(act):
        for q in range(n_cols):

            @pl.when((c == 0) & (r > 0))
            def _():
                act(main_copy(q, r - 1, half_rows, up_s.at[0, q]))
                act(halo_copy(q, r - 1, half_rows, up_s.at[1, q]))

            @pl.when(c != q)
            def _():
                act(main_copy(q, r, c, main_s.at[q]))
                act(halo_copy(q, r, c, halo_s.at[q]))

    outgoing(lambda copy: copy.start())

    load_x.wait()
    width = x.shape[2]
    sort = spread_matrix(width, False)
    for p in range(x.shape[0]):
        ordered = nn(x[p], sort).astype(BF16)
        for s in range(2):
            xt[p % 2, s, :, block(p // 2)] = ordered[:, block(s)]

    for i in range(half_rows + 1):
        if i < half_rows:
            arrives = c != i
        else:
            arrives = r < n_rows - 1

        @pl.when(arrives)
        def _():
            main_copy(0, r, i, main_s.at[0]).wait_recv()
            halo_copy(0, r, i, halo_s.at[0]).wait_recv()

    slots = half_rows + 1
    eye = ones_where(iota((chans, chans), 0) == iota((chans, chans), 1))
    turned = nt(eye, gh[...].reshape(slots * EDGE, chans)).astype(BF16)
    shift = ones_where(iota((half_cols, half_cols), 0) == iota((half_cols, half_cols), 1) + 1)
    for i in range(slots):
        place = (slots * EDGE, half_cols)
        last = (iota(place, 0) == i * EDGE + c) & (iota(place, 1) == half_cols - 1)
        gs[:, block(i)] = (nn(gm[:, block(i)], shift) + nn(turned, ones_where(last))).astype(BF16)

    def grad(down, along):
        src = gs if along else gm
        return src[:, down * half_cols : (down + half_rows) * half_cols]

    split = chans // 2
    part[2 * count - 1] = jnp.zeros(part.shape[1:], F32)
    for a in range(3):
        for b in range(3):
            t = 3 * a + b
            terms = nt(xt[PARITY[a], PARITY[b]], grad(SHIFT[a], SHIFT[b]))
            part[3 * t] = terms[:split, :LANES]
            part[3 * t + 1] = terms[split:, :LANES]
            part[3 * t + 2] = jnp.concatenate([terms[:split, LANES:], terms[split:, LANES:]], axis=1)

    def pair_copy(j):
        return pltpu.make_async_remote_copy(
            src_ref=part.at[(1 - core) * count + j], dst_ref=pair.at[j],
            send_sem=pair_s.at[j], recv_sem=pair_r.at[j], device_id=partner, device_id_type=MESH,
        )

    upper = chip // (chips // 2)
    half_count = count // 2

    def far_first(i):
        near = i // half_count
        side = upper * near + (1 - upper) * (1 - near)
        return side * half_count + lax.rem(chip + i, half_count)

    def owner_of(j):
        return (j * chips) // count

    for i in range(count):
        pair_copy(far_first(i)).start()

    piece = outbox.shape[1] // PIECES

    def cut(h):
        return pl.ds(h * piece, piece)

    def scatter_copy(j, h):
        owner = owner_of(j)
        return pltpu.make_async_remote_copy(
            src_ref=outbox.at[j, cut(h)], dst_ref=inbox.at[chip, cut(h)],
            send_sem=rs_s.at[h, j], recv_sem=rs_r.at[h, chip],
            device_id=(owner // depth, 2 * lax.rem(owner, depth) + core), device_id_type=MESH,
        )

    for i in range(count):
        j = far_first(i)
        pair_copy(j).wait_recv()
        outbox[j] = (part[base + j] + pair[j]).astype(BF16)

        @pl.when(chip != owner_of(j))
        def _():
            scatter_copy(j, 0).start()

    for h in range(1, PIECES):
        for i in range(count):
            j = far_first(i)

            @pl.when(chip != owner_of(j))
            def _():
                scatter_copy(j, h).start()

    load_w.wait()
    back = spread_matrix(width, True)

    def tap(a, b):
        return nn(w[a, b], grad(SHIFT[a], SHIFT[b]))

    for odd in range(2):
        taps = (0, 2) if odd else (1,)
        even_cols = sum(tap(a, 1) for a in taps).astype(BF16)
        odd_cols = sum(tap(a, 0) + tap(a, 2) for a in taps).astype(BF16)
        for i in range(half_rows):
            both = jnp.concatenate([even_cols[:, block(i)], odd_cols[:, block(i)]], axis=1)
            ig_ref[2 * i + odd] = nn(both, back).astype(BF16)

    plane = 2 * depth
    layers = chips // plane
    layer, spot = chip // plane, lax.rem(chip, plane)

    def chunk_of(other):
        return (other * count + chips - 1) // chips

    def owns(other):
        return (chunk_of(other) < count) & (owner_of(chunk_of(other)) == other)

    mine = chunk_of(chip)

    def share(j, h, row, col, send):
        return pltpu.make_async_remote_copy(
            src_ref=full.at[base + j, cut(h)], dst_ref=full.at[base + j, cut(h)],
            send_sem=send, recv_sem=ag_r.at[h, j], device_id=(row, col), device_id_type=MESH,
        )

    def to_layers(h, act):
        @pl.when(owns(chip))
        def _():
            for i in range(layers):
                other = lax.rem(layer + i + layers // 2, layers)

                @pl.when(other != layer)
                def _():
                    act(share(mine, h, 2 * other + spot // depth, c, ag_s.at[h, other]))

    def to_plane(source_layer, h, act):
        j = chunk_of(source_layer * plane + spot)
        for i in range(1, plane):
            other = lax.rem(spot + i, plane)
            act(share(
                j, h, 2 * layer + other // depth, 2 * lax.rem(other, depth) + core,
                plane_s.at[h, source_layer, other],
            ))

    def forward_copy(j, h, side):
        return pltpu.make_async_remote_copy(
            src_ref=full.at[side * count + j, cut(h)], dst_ref=full.at[side * count + j, cut(h)],
            send_sem=fw_s.at[h, j], recv_sem=fw_r.at[h, j], device_id=partner, device_id_type=MESH,
        )

    def pass_on(j, h):
        forward_copy(j, h, core).start()
        sum_ref[base + j, cut(h)] = full[base + j, cut(h)]

    def reduce(h):
        @pl.when(owns(chip))
        def _():
            def collect(i, total):
                source = lax.rem(chip + i, chips)
                pltpu.make_async_remote_copy(
                    src_ref=outbox.at[0, cut(h)], dst_ref=inbox.at[source, cut(h)],
                    send_sem=rs_s.at[h, 0], recv_sem=rs_r.at[h, source],
                    device_id=partner, device_id_type=MESH,
                ).wait_recv()
                return total + inbox[source, cut(h)].astype(F32)

            own = part[base + mine, cut(h)] + pair[mine, cut(h)]
            total = lax.fori_loop(1, chips, collect, own)
            full[base + mine, cut(h)] = (total * scale).astype(BF16)

        to_layers(h, lambda copy: copy.start())

        @pl.when(owns(chip))
        def _():
            to_plane(layer, h, lambda copy: copy.start())
            pass_on(mine, h)

    def relay(h):
        def step(i, _):
            source_layer = lax.rem(layer + i, layers)
            source = source_layer * plane + spot

            @pl.when(owns(source))
            def _():
                share(chunk_of(source), h, r, c, ag_s.at[h, layer]).wait_recv()
                to_plane(source_layer, h, lambda copy: copy.start())
                pass_on(chunk_of(source), h)

            return 0

        lax.fori_loop(1, layers, step, 0)

    def take(h):
        def step(i, _):
            source = lax.rem(layer + i // (plane - 1), layers) * plane + lax.rem(
                spot + 1 + lax.rem(i, plane - 1), plane
            )

            @pl.when(owns(source))
            def _():
                share(chunk_of(source), h, r, c, ag_s.at[h, layer]).wait_recv()
                pass_on(chunk_of(source), h)

            return 0

        lax.fori_loop(0, layers * (plane - 1), step, 0)

    reduce(0)
    for h in range(PIECES):
        relay(h)
        if h + 1 < PIECES:
            reduce(h + 1)
        take(h)

    for h in range(PIECES):
        for j in range(count):
            forward_copy(j, h, 1 - core).wait_recv()
            sum_ref[(1 - core) * count + j, cut(h)] = full[(1 - core) * count + j, cut(h)]

    outgoing(lambda copy: copy.wait_send())
    for j in range(count):
        pair_copy(j).wait_send()

    for h in range(PIECES):
        for j in range(count):
            forward_copy(j, h, core).wait_send()

            @pl.when(chip != owner_of(j))
            def _():
                scatter_copy(j, h).wait_send()

        to_layers(h, lambda copy: copy.wait_send())

        def sent(i, _):
            @pl.when(owns(i * plane + spot))
            def _():
                to_plane(i, h, lambda copy: copy.wait_send())

            return 0

        lax.fori_loop(0, layers, sent, 0)


def unpack_kernel(ig_ref, sum_ref, ig_out, filter_out, wide, sems):
    split = wide.shape[1] // 2
    rest = wide.shape[2] - LANES
    taps = wide.shape[0]
    whole = pltpu.make_async_copy(ig_ref, ig_out, sems.at[taps])
    whole.start()
    copies = []
    for t in range(taps):
        wide[t, :split, :LANES] = sum_ref[3 * t].astype(F32)
        wide[t, split:, :LANES] = sum_ref[3 * t + 1].astype(F32)
        packed = sum_ref[3 * t + 2].astype(F32)
        wide[t, :split, LANES:] = packed[:, :rest]
        wide[t, split:, LANES:] = packed[:, rest:]
        copies.append(pltpu.make_async_copy(wide.at[t], filter_out.at[t], sems.at[t]))
        copies[-1].start()
    whole.wait()
    for copy in copies:
        copy.wait()


def per_device(n_rows, n_cols, grad_out, inputs, weight):
    rows_local, cols_local, chans = inputs.shape
    grad_out, inputs = (jnp.swapaxes(grad_out, 1, 2), jnp.swapaxes(inputs, 1, 2))
    grad_out = pltpu.with_memory_space_constraint(grad_out, pltpu.HBM)
    inputs = pltpu.with_memory_space_constraint(inputs, pltpu.HBM)
    weight = pltpu.with_memory_space_constraint(weight, pltpu.HBM)
    half_rows, half_cols = rows_local // 2, cols_local // 2
    split = chans // 2
    chips = n_rows * n_cols // 2
    count = (27 + 1) // 2
    scale = 1.0 / math.sqrt(half_rows * n_rows * half_cols * n_cols)
    dma = pltpu.SemaphoreType.DMA
    vmem = pl.BlockSpec(memory_space=pltpu.VMEM)
    anywhere = pl.BlockSpec(memory_space=pl.ANY)
    hbm = pl.BlockSpec(memory_space=pltpu.HBM)
    input_grad, sums = pl.pallas_call(
        functools.partial(step_kernel, n_rows, n_cols, scale),
        out_shape=(
            jax.ShapeDtypeStruct(inputs.shape, BF16),
            jax.ShapeDtypeStruct((2 * count, split, LANES), BF16),
        ),
        in_specs=[hbm, hbm, hbm],
        out_specs=(vmem, vmem),
        scratch_shapes=[
            pltpu.VMEM(grad_out.shape, BF16),
            pltpu.VMEM(inputs.shape, BF16),
            pltpu.VMEM(weight.shape, BF16),
            pltpu.VMEM((chans, (half_rows + 1) * half_cols), BF16),
            pltpu.VMEM((half_rows + 1, EDGE, chans), BF16),
            pltpu.VMEM((chans, (half_rows + 1) * half_cols), BF16),
            pltpu.VMEM((EDGE, chans), BF16),
            pltpu.VMEM((2, 2, chans, half_rows * half_cols), BF16),
            pltpu.VMEM((2 * count, split, LANES), F32),
            pltpu.VMEM((count, split, LANES), F32),
            pltpu.VMEM((count, split, LANES), BF16),
            pltpu.VMEM((chips, split, LANES), BF16),
            pltpu.VMEM((2 * count, split, LANES), BF16),
            dma((3,)),
            dma((n_cols,)), dma((half_rows + 1,)), dma((n_cols,)), dma((half_rows + 1,)), dma((2, n_cols)),
            dma((count,)), dma((count,)),
            dma((PIECES, count)), dma((PIECES, chips)), dma((PIECES, chips)), dma((PIECES, count)),
            dma((PIECES, chips // n_cols, n_cols)), dma((PIECES, count)), dma((PIECES, count)),
        ],
        compiler_params=pltpu.CompilerParams(
            collective_id=0, has_side_effects=True, vmem_limit_bytes=48 * 1024 * 1024
        ),
    )(grad_out, inputs, weight)
    input_grad, filter_grad = pl.pallas_call(
        unpack_kernel,
        out_shape=(
            jax.ShapeDtypeStruct(inputs.shape, BF16),
            jax.ShapeDtypeStruct((9, chans, chans), F32),
        ),
        in_specs=[vmem, vmem],
        out_specs=(anywhere, anywhere),
        scratch_shapes=[pltpu.VMEM((9, chans, chans), F32), dma((10,))],
        compiler_params=pltpu.CompilerParams(vmem_limit_bytes=12 * 1024 * 1024),
    )(input_grad, sums)
    return jnp.swapaxes(input_grad, 1, 2), filter_grad.reshape(3, 3, chans, chans)


def solution(mesh):
    in_specs = (P(("rows", "cols"), None, None), P("rows", "cols", None), P())
    out_specs = (P("rows", "cols", None), P())
    return jax.shard_map(
        functools.partial(per_device, mesh.shape["rows"], mesh.shape["cols"]),
        mesh=mesh, in_specs=in_specs, out_specs=out_specs, check_vma=False,
    )
```

```python
import functools
import math

import jax
import jax.numpy as jnp
from jax import lax
from jax.experimental import pallas as pl
from jax.experimental.pallas import tpu as pltpu
from jax.sharding import PartitionSpec as P

MESH = pl.DeviceIdType.MESH
LANES = 128
EDGE = 16
PIECES = 1
F32 = jnp.float32
BF16 = jnp.bfloat16
PARITY = (1, 0, 1)
SHIFT = (1, 0, 0)


def iota(shape, dim):
    return lax.broadcasted_iota(jnp.int32, shape, dim)


def ones_where(mask):
    return jnp.where(mask, 1.0, 0.0).astype(BF16)


def spread_matrix(size, back):
    half = size // 2
    i = iota((size, size), 0 if back else 1)
    k = iota((size, size), 1 if back else 0)
    return ones_where(k == jnp.where(i < half, 2 * i, 2 * (i - half) + 1))


def nn(a, b):
    return jnp.dot(a, b, preferred_element_type=F32)


def nt(a, b):
    return lax.dot_general(a, b, (((1,), (1,)), ((), ())), preferred_element_type=F32)


def step_kernel(
    n_rows, n_cols, scale,
    g_hbm, x_hbm, w_hbm, ig_ref, sum_ref,
    g_ref, x, w, gm, gh, gs, edge, xt, part, pair, outbox, inbox, full,
    load_sem, main_s, main_r, halo_s, halo_r, up_s, pair_s, pair_r,
    rs_s, rs_r, ag_s, ag_r, plane_s, fw_s, fw_r,
):
    r = lax.axis_index("rows")
    c = lax.axis_index("cols")
    core = lax.rem(c, 2)
    depth = n_cols // 2
    chips = n_rows * depth
    chip = r * depth + c // 2
    partner = (r, c + 1 - 2 * core)
    half_rows = n_cols
    half_cols = g_ref.shape[2] // n_cols
    chans = g_ref.shape[1]
    count = outbox.shape[0]
    base = core * count
    devices = n_rows * n_cols
    me = r * n_cols + c

    barrier = pltpu.get_barrier_semaphore()

    def greet(i, _):
        other = lax.rem(me + i, devices)
        pl.semaphore_signal(
            barrier, inc=1, device_id=(other // n_cols, lax.rem(other, n_cols)), device_id_type=MESH
        )
        return 0

    lax.fori_loop(1, devices, greet, 0)
    load_x = pltpu.make_async_copy(x_hbm, x, load_sem.at[0])
    load_w = pltpu.make_async_copy(w_hbm, w, load_sem.at[1])
    load_g = pltpu.make_async_copy(g_hbm, g_ref, load_sem.at[2])
    load_g.start()
    load_x.start()
    load_w.start()

    def block(i):
        return slice(i * half_cols, (i + 1) * half_cols)

    @pl.when(r == n_rows - 1)
    def _():
        gm[:, block(half_rows)] = jnp.zeros((chans, half_cols), BF16)
        gh[half_rows] = jnp.zeros(gh.shape[1:], BF16)

    load_g.wait()
    for q in range(n_cols):

        @pl.when(c == q)
        def _():
            gm[:, block(q)] = g_ref[0, :, block(q)]

    full_cols = g_ref.shape[2]
    wanted = (iota((EDGE, full_cols), 0) + 1) * half_cols
    edge[...] = nt(ones_where(wanted == iota((EDGE, full_cols), 1)), g_ref[0]).astype(BF16)
    gh[c] = edge[...]

    pl.semaphore_wait(barrier, devices - 1)

    def main_copy(q, row, slot, send):
        return pltpu.make_async_remote_copy(
            src_ref=g_ref.at[0, :, pl.ds(q * half_cols, half_cols)],
            dst_ref=gm.at[:, pl.ds(pl.multiple_of(slot * half_cols, LANES), half_cols)],
            send_sem=send, recv_sem=main_r.at[slot], device_id=(row, q), device_id_type=MESH,
        )

    def halo_copy(q, row, slot, send):
        return pltpu.make_async_remote_copy(
            src_ref=edge, dst_ref=gh.at[slot],
            send_sem=send, recv_sem=halo_r.at[slot], device_id=(row, q), device_id_type=MESH,
        )

    def outgoing(act):
        for q in range(n_cols):

            @pl.when((c == 0) & (r > 0))
            def _():
                act(main_copy(q, r - 1, half_rows, up_s.at[0, q]))
                act(halo_copy(q, r - 1, half_rows, up_s.at[1, q]))

            @pl.when(c != q)
            def _():
                act(main_copy(q, r, c, main_s.at[q]))
                act(halo_copy(q, r, c, halo_s.at[q]))

    outgoing(lambda copy: copy.start())

    load_x.wait()
    width = x.shape[2]
    sort = spread_matrix(width, False)
    for p in range(x.shape[0]):
        ordered = nn(x[p], sort).astype(BF16)
        for s in range(2):
            xt[p % 2, s, :, block(p // 2)] = ordered[:, block(s)]

    for i in range(half_rows + 1):
        if i < half_rows:
            arrives = c != i
        else:
            arrives = r < n_rows - 1

        @pl.when(arrives)
        def _():
            main_copy(0, r, i, main_s.at[0]).wait_recv()
            halo_copy(0, r, i, halo_s.at[0]).wait_recv()

    slots = half_rows + 1
    eye = ones_where(iota((chans, chans), 0) == iota((chans, chans), 1))
    turned = nt(eye, gh[...].reshape(slots * EDGE, chans)).astype(BF16)
    shift = ones_where(iota((half_cols, half_cols), 0) == iota((half_cols, half_cols), 1) + 1)
    for i in range(slots):
        place = (slots * EDGE, half_cols)
        last = (iota(place, 0) == i * EDGE + c) & (iota(place, 1) == half_cols - 1)
        gs[:, block(i)] = (nn(gm[:, block(i)], shift) + nn(turned, ones_where(last))).astype(BF16)

    def grad(down, along):
        src = gs if along else gm
        return src[:, down * half_cols : (down + half_rows) * half_cols]

    split = chans // 2
    part[2 * count - 1] = jnp.zeros(part.shape[1:], F32)
    for a in range(3):
        for b in range(3):
            t = 3 * a + b
            terms = nt(xt[PARITY[a], PARITY[b]], grad(SHIFT[a], SHIFT[b]))
            part[3 * t] = terms[:split, :LANES]
            part[3 * t + 1] = terms[split:, :LANES]
            part[3 * t + 2] = jnp.concatenate([terms[:split, LANES:], terms[split:, LANES:]], axis=1)

    def pair_copy(j):
        return pltpu.make_async_remote_copy(
            src_ref=part.at[(1 - core) * count + j], dst_ref=pair.at[j],
            send_sem=pair_s.at[j], recv_sem=pair_r.at[j], device_id=partner, device_id_type=MESH,
        )

    upper = chip // (chips // 2)
    half_count = count // 2

    def far_first(i):
        near = i // half_count
        side = upper * near + (1 - upper) * (1 - near)
        return side * half_count + lax.rem(chip + i, half_count)

    def owner_of(j):
        return (j * chips) // count

    for i in range(count):
        pair_copy(far_first(i)).start()

    piece = outbox.shape[1] // PIECES

    def cut(h):
        return pl.ds(h * piece, piece)

    def scatter_copy(j, h):
        owner = owner_of(j)
        return pltpu.make_async_remote_copy(
            src_ref=outbox.at[j, cut(h)], dst_ref=inbox.at[chip, cut(h)],
            send_sem=rs_s.at[h, j], recv_sem=rs_r.at[h, chip],
            device_id=(owner // depth, 2 * lax.rem(owner, depth) + core), device_id_type=MESH,
        )

    for i in range(count):
        j = far_first(i)
        pair_copy(j).wait_recv()
        outbox[j] = (part[base + j] + pair[j]).astype(BF16)

        @pl.when(chip != owner_of(j))
        def _():
            scatter_copy(j, 0).start()

    for h in range(1, PIECES):
        for i in range(count):
            j = far_first(i)

            @pl.when(chip != owner_of(j))
            def _():
                scatter_copy(j, h).start()

    load_w.wait()
    back = spread_matrix(width, True)

    def tap(a, b):
        return nn(w[a, b], grad(SHIFT[a], SHIFT[b]))

    for odd in range(2):
        taps = (0, 2) if odd else (1,)
        even_cols = sum(tap(a, 1) for a in taps).astype(BF16)
        odd_cols = sum(tap(a, 0) + tap(a, 2) for a in taps).astype(BF16)
        for i in range(half_rows):
            both = jnp.concatenate([even_cols[:, block(i)], odd_cols[:, block(i)]], axis=1)
            ig_ref[2 * i + odd] = nn(both, back).astype(BF16)

    plane = 2 * depth
    layers = chips // plane
    layer, spot = chip // plane, lax.rem(chip, plane)

    def chunk_of(other):
        return (other * count + chips - 1) // chips

    def owns(other):
        return (chunk_of(other) < count) & (owner_of(chunk_of(other)) == other)

    mine = chunk_of(chip)

    def share(j, h, row, col, send):
        return pltpu.make_async_remote_copy(
            src_ref=full.at[base + j, cut(h)], dst_ref=full.at[base + j, cut(h)],
            send_sem=send, recv_sem=ag_r.at[h, j], device_id=(row, col), device_id_type=MESH,
        )

    def to_layers(h, act):
        @pl.when(owns(chip))
        def _():
            for i in range(layers):
                other = lax.rem(layer + i, layers)

                @pl.when(other != layer)
                def _():
                    act(share(mine, h, 2 * other + spot // depth, c, ag_s.at[h, other]))

    def to_plane(source_layer, h, act):
        j = chunk_of(source_layer * plane + spot)
        for i in range(1, plane):
            other = lax.rem(spot + i, plane)
            act(share(
                j, h, 2 * layer + other // depth, 2 * lax.rem(other, depth) + core,
                plane_s.at[h, source_layer, other],
            ))

    def forward_copy(j, h, side):
        return pltpu.make_async_remote_copy(
            src_ref=full.at[side * count + j, cut(h)], dst_ref=full.at[side * count + j, cut(h)],
            send_sem=fw_s.at[h, j], recv_sem=fw_r.at[h, j], device_id=partner, device_id_type=MESH,
        )

    def pass_on(j, h):
        forward_copy(j, h, core).start()
        sum_ref[base + j, cut(h)] = full[base + j, cut(h)]

    def reduce(h):
        @pl.when(owns(chip))
        def _():
            def collect(i, total):
                source = lax.rem(chip + i, chips)
                pltpu.make_async_remote_copy(
                    src_ref=outbox.at[0, cut(h)], dst_ref=inbox.at[source, cut(h)],
                    send_sem=rs_s.at[h, 0], recv_sem=rs_r.at[h, source],
                    device_id=partner, device_id_type=MESH,
                ).wait_recv()
                return total + inbox[source, cut(h)].astype(F32)

            own = part[base + mine, cut(h)] + pair[mine, cut(h)]
            total = lax.fori_loop(1, chips, collect, own)
            full[base + mine, cut(h)] = (total * scale).astype(BF16)

        to_layers(h, lambda copy: copy.start())

        @pl.when(owns(chip))
        def _():
            to_plane(layer, h, lambda copy: copy.start())
            pass_on(mine, h)

    def relay(h):
        def step(i, _):
            source_layer = lax.rem(layer + i, layers)
            source = source_layer * plane + spot

            @pl.when(owns(source))
            def _():
                share(chunk_of(source), h, r, c, ag_s.at[h, layer]).wait_recv()
                to_plane(source_layer, h, lambda copy: copy.start())
                pass_on(chunk_of(source), h)

            return 0

        lax.fori_loop(1, layers, step, 0)

    def take(h):
        def step(i, _):
            source = lax.rem(layer + i // (plane - 1), layers) * plane + lax.rem(
                spot + 1 + lax.rem(i, plane - 1), plane
            )

            @pl.when(owns(source))
            def _():
                share(chunk_of(source), h, r, c, ag_s.at[h, layer]).wait_recv()
                pass_on(chunk_of(source), h)

            return 0

        lax.fori_loop(0, layers * (plane - 1), step, 0)

    reduce(0)
    for h in range(PIECES):
        relay(h)
        if h + 1 < PIECES:
            reduce(h + 1)
        take(h)

    for h in range(PIECES):
        for j in range(count):
            forward_copy(j, h, 1 - core).wait_recv()
            sum_ref[(1 - core) * count + j, cut(h)] = full[(1 - core) * count + j, cut(h)]

    outgoing(lambda copy: copy.wait_send())
    for j in range(count):
        pair_copy(j).wait_send()

    for h in range(PIECES):
        for j in range(count):
            forward_copy(j, h, core).wait_send()

            @pl.when(chip != owner_of(j))
            def _():
                scatter_copy(j, h).wait_send()

        to_layers(h, lambda copy: copy.wait_send())

        def sent(i, _):
            @pl.when(owns(i * plane + spot))
            def _():
                to_plane(i, h, lambda copy: copy.wait_send())

            return 0

        lax.fori_loop(0, layers, sent, 0)


def unpack_kernel(ig_ref, sum_ref, ig_out, filter_out, wide, sems):
    split = wide.shape[1] // 2
    rest = wide.shape[2] - LANES
    taps = wide.shape[0]
    whole = pltpu.make_async_copy(ig_ref, ig_out, sems.at[taps])
    whole.start()
    copies = []
    for t in range(taps):
        wide[t, :split, :LANES] = sum_ref[3 * t].astype(F32)
        wide[t, split:, :LANES] = sum_ref[3 * t + 1].astype(F32)
        packed = sum_ref[3 * t + 2].astype(F32)
        wide[t, :split, LANES:] = packed[:, :rest]
        wide[t, split:, LANES:] = packed[:, rest:]
        copies.append(pltpu.make_async_copy(wide.at[t], filter_out.at[t], sems.at[t]))
        copies[-1].start()
    whole.wait()
    for copy in copies:
        copy.wait()


def per_device(n_rows, n_cols, grad_out, inputs, weight):
    rows_local, cols_local, chans = inputs.shape
    grad_out, inputs = (jnp.swapaxes(grad_out, 1, 2), jnp.swapaxes(inputs, 1, 2))
    grad_out = pltpu.with_memory_space_constraint(grad_out, pltpu.HBM)
    inputs = pltpu.with_memory_space_constraint(inputs, pltpu.HBM)
    weight = pltpu.with_memory_space_constraint(weight, pltpu.HBM)
    half_rows, half_cols = rows_local // 2, cols_local // 2
    split = chans // 2
    chips = n_rows * n_cols // 2
    count = (27 + 1) // 2
    scale = 1.0 / math.sqrt(half_rows * n_rows * half_cols * n_cols)
    dma = pltpu.SemaphoreType.DMA
    vmem = pl.BlockSpec(memory_space=pltpu.VMEM)
    anywhere = pl.BlockSpec(memory_space=pl.ANY)
    hbm = pl.BlockSpec(memory_space=pltpu.HBM)
    input_grad, sums = pl.pallas_call(
        functools.partial(step_kernel, n_rows, n_cols, scale),
        out_shape=(
            jax.ShapeDtypeStruct(inputs.shape, BF16),
            jax.ShapeDtypeStruct((2 * count, split, LANES), BF16),
        ),
        in_specs=[hbm, hbm, hbm],
        out_specs=(vmem, vmem),
        scratch_shapes=[
            pltpu.VMEM(grad_out.shape, BF16),
            pltpu.VMEM(inputs.shape, BF16),
            pltpu.VMEM(weight.shape, BF16),
            pltpu.VMEM((chans, (half_rows + 1) * half_cols), BF16),
            pltpu.VMEM((half_rows + 1, EDGE, chans), BF16),
            pltpu.VMEM((chans, (half_rows + 1) * half_cols), BF16),
            pltpu.VMEM((EDGE, chans), BF16),
            pltpu.VMEM((2, 2, chans, half_rows * half_cols), BF16),
            pltpu.VMEM((2 * count, split, LANES), F32),
            pltpu.VMEM((count, split, LANES), F32),
            pltpu.VMEM((count, split, LANES), BF16),
            pltpu.VMEM((chips, split, LANES), BF16),
            pltpu.VMEM((2 * count, split, LANES), BF16),
            dma((3,)),
            dma((n_cols,)), dma((half_rows + 1,)), dma((n_cols,)), dma((half_rows + 1,)), dma((2, n_cols)),
            dma((count,)), dma((count,)),
            dma((PIECES, count)), dma((PIECES, chips)), dma((PIECES, chips)), dma((PIECES, count)),
            dma((PIECES, chips // n_cols, n_cols)), dma((PIECES, count)), dma((PIECES, count)),
        ],
        compiler_params=pltpu.CompilerParams(
            collective_id=0, has_side_effects=True, vmem_limit_bytes=48 * 1024 * 1024
        ),
    )(grad_out, inputs, weight)
    input_grad, filter_grad = pl.pallas_call(
        unpack_kernel,
        out_shape=(
            jax.ShapeDtypeStruct(inputs.shape, BF16),
            jax.ShapeDtypeStruct((9, chans, chans), F32),
        ),
        in_specs=[vmem, vmem],
        out_specs=(anywhere, anywhere),
        scratch_shapes=[pltpu.VMEM((9, chans, chans), F32), dma((10,))],
        compiler_params=pltpu.CompilerParams(vmem_limit_bytes=12 * 1024 * 1024),
    )(input_grad, sums)
    return jnp.swapaxes(input_grad, 1, 2), filter_grad.reshape(3, 3, chans, chans)


def solution(mesh):
    in_specs = (P(("rows", "cols"), None, None), P("rows", "cols", None), P())
    out_specs = (P("rows", "cols", None), P())
    return jax.shard_map(
        functools.partial(per_device, mesh.shape["rows"], mesh.shape["cols"]),
        mesh=mesh, in_specs=in_specs, out_specs=out_specs, check_vma=False,
    )
```

```python
import functools
import math

import jax
import jax.numpy as jnp
from jax import lax
from jax.experimental import pallas as pl
from jax.experimental.pallas import tpu as pltpu
from jax.sharding import PartitionSpec as P

MESH = pl.DeviceIdType.MESH
LANES = 128
EDGE = 16
PIECES = 1
F32 = jnp.float32
BF16 = jnp.bfloat16
PARITY = (1, 0, 1)
SHIFT = (1, 0, 0)


def iota(shape, dim):
    return lax.broadcasted_iota(jnp.int32, shape, dim)


def ones_where(mask):
    return jnp.where(mask, 1.0, 0.0).astype(BF16)


def spread_matrix(size, back):
    half = size // 2
    i = iota((size, size), 0 if back else 1)
    k = iota((size, size), 1 if back else 0)
    return ones_where(k == jnp.where(i < half, 2 * i, 2 * (i - half) + 1))


def nn(a, b):
    return jnp.dot(a, b, preferred_element_type=F32)


def nt(a, b):
    return lax.dot_general(a, b, (((1,), (1,)), ((), ())), preferred_element_type=F32)


def step_kernel(
    n_rows, n_cols, scale,
    g_hbm, x_hbm, w_hbm, ig_ref, sum_ref,
    g_ref, x, w, gm, gh, gs, edge, xt, part, pair, outbox, inbox, full,
    load_sem, main_s, main_r, halo_s, halo_r, up_s, pair_s, pair_r,
    rs_s, rs_r, ag_s, ag_r, plane_s, fw_s, fw_r,
):
    r = lax.axis_index("rows")
    c = lax.axis_index("cols")
    core = lax.rem(c, 2)
    depth = n_cols // 2
    chips = n_rows * depth
    chip = r * depth + c // 2
    partner = (r, c + 1 - 2 * core)
    half_rows = n_cols
    half_cols = g_ref.shape[2] // n_cols
    chans = g_ref.shape[1]
    count = outbox.shape[0]
    base = core * count
    devices = n_rows * n_cols
    me = r * n_cols + c

    barrier = pltpu.get_barrier_semaphore()

    def greet(i, _):
        other = lax.rem(me + i, devices)
        pl.semaphore_signal(
            barrier, inc=1, device_id=(other // n_cols, lax.rem(other, n_cols)), device_id_type=MESH
        )
        return 0

    lax.fori_loop(1, devices, greet, 0)
    load_x = pltpu.make_async_copy(x_hbm, x, load_sem.at[0])
    load_w = pltpu.make_async_copy(w_hbm, w, load_sem.at[1])
    load_g = pltpu.make_async_copy(g_hbm, g_ref, load_sem.at[2])
    load_g.start()
    load_x.start()
    load_w.start()

    def block(i):
        return slice(i * half_cols, (i + 1) * half_cols)

    @pl.when(r == n_rows - 1)
    def _():
        gm[:, block(half_rows)] = jnp.zeros((chans, half_cols), BF16)
        gh[half_rows] = jnp.zeros(gh.shape[1:], BF16)

    load_g.wait()
    for q in range(n_cols):

        @pl.when(c == q)
        def _():
            gm[:, block(q)] = g_ref[0, :, block(q)]

    full_cols = g_ref.shape[2]
    wanted = (iota((EDGE, full_cols), 0) + 1) * half_cols
    edge[...] = nt(ones_where(wanted == iota((EDGE, full_cols), 1)), g_ref[0]).astype(BF16)
    gh[c] = edge[...]

    pl.semaphore_wait(barrier, devices - 1)

    def main_copy(q, row, slot, send):
        return pltpu.make_async_remote_copy(
            src_ref=g_ref.at[0, :, pl.ds(q * half_cols, half_cols)],
            dst_ref=gm.at[:, pl.ds(pl.multiple_of(slot * half_cols, LANES), half_cols)],
            send_sem=send, recv_sem=main_r.at[slot], device_id=(row, q), device_id_type=MESH,
        )

    def halo_copy(q, row, slot, send):
        return pltpu.make_async_remote_copy(
            src_ref=edge, dst_ref=gh.at[slot],
            send_sem=send, recv_sem=halo_r.at[slot], device_id=(row, q), device_id_type=MESH,
        )

    def outgoing(act):
        for q in range(n_cols):

            @pl.when((c == 0) & (r > 0))
            def _():
                act(main_copy(q, r - 1, half_rows, up_s.at[0, q]))
                act(halo_copy(q, r - 1, half_rows, up_s.at[1, q]))

            @pl.when(c != q)
            def _():
                act(main_copy(q, r, c, main_s.at[q]))
                act(halo_copy(q, r, c, halo_s.at[q]))

    outgoing(lambda copy: copy.start())

    load_x.wait()
    width = x.shape[2]
    sort = spread_matrix(width, False)
    for p in range(x.shape[0]):
        ordered = nn(x[p], sort).astype(BF16)
        for s in range(2):
            xt[p % 2, s, :, block(p // 2)] = ordered[:, block(s)]

    for i in range(half_rows + 1):
        if i < half_rows:
            arrives = c != i
        else:
            arrives = r < n_rows - 1

        @pl.when(arrives)
        def _():
            main_copy(0, r, i, main_s.at[0]).wait_recv()
            halo_copy(0, r, i, halo_s.at[0]).wait_recv()

    slots = half_rows + 1
    eye = ones_where(iota((chans, chans), 0) == iota((chans, chans), 1))
    turned = nt(eye, gh[...].reshape(slots * EDGE, chans)).astype(BF16)
    shift = ones_where(iota((half_cols, half_cols), 0) == iota((half_cols, half_cols), 1) + 1)
    for i in range(slots):
        place = (slots * EDGE, half_cols)
        last = (iota(place, 0) == i * EDGE + c) & (iota(place, 1) == half_cols - 1)
        gs[:, block(i)] = (nn(gm[:, block(i)], shift) + nn(turned, ones_where(last))).astype(BF16)

    def grad(down, along):
        src = gs if along else gm
        return src[:, down * half_cols : (down + half_rows) * half_cols]

    split = chans // 2
    part[2 * count - 1] = jnp.zeros(part.shape[1:], F32)
    for a in range(3):
        for b in range(3):
            t = 3 * a + b
            terms = nt(xt[PARITY[a], PARITY[b]], grad(SHIFT[a], SHIFT[b]))
            part[3 * t] = terms[:split, :LANES]
            part[3 * t + 1] = terms[split:, :LANES]
            part[3 * t + 2] = jnp.concatenate([terms[:split, LANES:], terms[split:, LANES:]], axis=1)

    def pair_copy(j):
        return pltpu.make_async_remote_copy(
            src_ref=part.at[(1 - core) * count + j], dst_ref=pair.at[j],
            send_sem=pair_s.at[j], recv_sem=pair_r.at[j], device_id=partner, device_id_type=MESH,
        )

    upper = chip // (chips // 2)
    half_count = count // 2

    def far_first(i):
        near = i // half_count
        side = upper * near + (1 - upper) * (1 - near)
        return side * half_count + lax.rem(chip + i, half_count)

    def owner_of(j):
        return (j * chips) // count

    for i in range(count):
        pair_copy(far_first(i)).start()

    piece = outbox.shape[1] // PIECES

    def cut(h):
        return pl.ds(h * piece, piece)

    def scatter_copy(j, h):
        owner = owner_of(j)
        return pltpu.make_async_remote_copy(
            src_ref=outbox.at[j, cut(h)], dst_ref=inbox.at[chip, cut(h)],
            send_sem=rs_s.at[h, j], recv_sem=rs_r.at[h, chip],
            device_id=(owner // depth, 2 * lax.rem(owner, depth) + core), device_id_type=MESH,
        )

    for i in range(count):
        j = far_first(i)
        pair_copy(j).wait_recv()
        outbox[j] = (part[base + j] + pair[j]).astype(BF16)

        @pl.when((chip != owner_of(j)) & (base + j < 27))
        def _():
            scatter_copy(j, 0).start()

    for h in range(1, PIECES):
        for i in range(count):
            j = far_first(i)

            @pl.when((chip != owner_of(j)) & (base + j < 27))
            def _():
                scatter_copy(j, h).start()

    load_w.wait()
    back = spread_matrix(width, True)

    def tap(a, b):
        return nn(w[a, b], grad(SHIFT[a], SHIFT[b]))

    for odd in range(2):
        taps = (0, 2) if odd else (1,)
        even_cols = sum(tap(a, 1) for a in taps).astype(BF16)
        odd_cols = sum(tap(a, 0) + tap(a, 2) for a in taps).astype(BF16)
        for i in range(half_rows):
            both = jnp.concatenate([even_cols[:, block(i)], odd_cols[:, block(i)]], axis=1)
            ig_ref[2 * i + odd] = nn(both, back).astype(BF16)

    plane = 2 * depth
    layers = chips // plane
    layer, spot = chip // plane, lax.rem(chip, plane)

    def chunk_of(other):
        return (other * count + chips - 1) // chips

    def owns(other):
        return (base + chunk_of(other) < 27) & (chunk_of(other) < count) & (owner_of(chunk_of(other)) == other)

    mine = chunk_of(chip)

    def share(j, h, row, col, send):
        return pltpu.make_async_remote_copy(
            src_ref=full.at[base + j, cut(h)], dst_ref=full.at[base + j, cut(h)],
            send_sem=send, recv_sem=ag_r.at[h, j], device_id=(row, col), device_id_type=MESH,
        )

    def to_layers(h, act):
        @pl.when(owns(chip))
        def _():
            for i in range(layers):
                other = lax.rem(layer + i, layers)

                @pl.when(other != layer)
                def _():
                    act(share(mine, h, 2 * other + spot // depth, c, ag_s.at[h, other]))

    def to_plane(source_layer, h, act):
        j = chunk_of(source_layer * plane + spot)
        for i in range(1, plane):
            other = lax.rem(spot + i, plane)
            act(share(
                j, h, 2 * layer + other // depth, 2 * lax.rem(other, depth) + core,
                plane_s.at[h, source_layer, other],
            ))

    def forward_copy(j, h, side):
        return pltpu.make_async_remote_copy(
            src_ref=full.at[side * count + j, cut(h)], dst_ref=full.at[side * count + j, cut(h)],
            send_sem=fw_s.at[h, j], recv_sem=fw_r.at[h, j], device_id=partner, device_id_type=MESH,
        )

    def pass_on(j, h):
        forward_copy(j, h, core).start()
        sum_ref[base + j, cut(h)] = full[base + j, cut(h)]

    def reduce(h):
        @pl.when(owns(chip))
        def _():
            def collect(i, total):
                source = lax.rem(chip + i, chips)
                pltpu.make_async_remote_copy(
                    src_ref=outbox.at[0, cut(h)], dst_ref=inbox.at[source, cut(h)],
                    send_sem=rs_s.at[h, 0], recv_sem=rs_r.at[h, source],
                    device_id=partner, device_id_type=MESH,
                ).wait_recv()
                return total + inbox[source, cut(h)].astype(F32)

            own = part[base + mine, cut(h)] + pair[mine, cut(h)]
            total = lax.fori_loop(1, chips, collect, own)
            full[base + mine, cut(h)] = (total * scale).astype(BF16)

        to_layers(h, lambda copy: copy.start())

        @pl.when(owns(chip))
        def _():
            to_plane(layer, h, lambda copy: copy.start())
            pass_on(mine, h)

    def relay(h):
        def step(i, _):
            source_layer = lax.rem(layer + i, layers)
            source = source_layer * plane + spot

            @pl.when(owns(source))
            def _():
                share(chunk_of(source), h, r, c, ag_s.at[h, layer]).wait_recv()
                to_plane(source_layer, h, lambda copy: copy.start())
                pass_on(chunk_of(source), h)

            return 0

        lax.fori_loop(1, layers, step, 0)

    def take(h):
        def step(i, _):
            source = lax.rem(layer + i // (plane - 1), layers) * plane + lax.rem(
                spot + 1 + lax.rem(i, plane - 1), plane
            )

            @pl.when(owns(source))
            def _():
                share(chunk_of(source), h, r, c, ag_s.at[h, layer]).wait_recv()
                pass_on(chunk_of(source), h)

            return 0

        lax.fori_loop(0, layers * (plane - 1), step, 0)

    reduce(0)
    for h in range(PIECES):
        relay(h)
        if h + 1 < PIECES:
            reduce(h + 1)
        take(h)

    for h in range(PIECES):
        for j in range(count):
            @pl.when((1 - core) * count + j < 27)
            def _():
                forward_copy(j, h, 1 - core).wait_recv()
                sum_ref[(1 - core) * count + j, cut(h)] = full[(1 - core) * count + j, cut(h)]

    outgoing(lambda copy: copy.wait_send())
    for j in range(count):
        pair_copy(j).wait_send()

    for h in range(PIECES):
        for j in range(count):
            @pl.when(base + j < 27)
            def _():
                forward_copy(j, h, core).wait_send()

            @pl.when((chip != owner_of(j)) & (base + j < 27))
            def _():
                scatter_copy(j, h).wait_send()

        to_layers(h, lambda copy: copy.wait_send())

        def sent(i, _):
            @pl.when(owns(i * plane + spot))
            def _():
                to_plane(i, h, lambda copy: copy.wait_send())

            return 0

        lax.fori_loop(0, layers, sent, 0)


def unpack_kernel(ig_ref, sum_ref, ig_out, filter_out, wide, sems):
    split = wide.shape[1] // 2
    rest = wide.shape[2] - LANES
    taps = wide.shape[0]
    whole = pltpu.make_async_copy(ig_ref, ig_out, sems.at[taps])
    whole.start()
    copies = []
    for t in range(taps):
        wide[t, :split, :LANES] = sum_ref[3 * t].astype(F32)
        wide[t, split:, :LANES] = sum_ref[3 * t + 1].astype(F32)
        packed = sum_ref[3 * t + 2].astype(F32)
        wide[t, :split, LANES:] = packed[:, :rest]
        wide[t, split:, LANES:] = packed[:, rest:]
        copies.append(pltpu.make_async_copy(wide.at[t], filter_out.at[t], sems.at[t]))
        copies[-1].start()
    whole.wait()
    for copy in copies:
        copy.wait()


def per_device(n_rows, n_cols, grad_out, inputs, weight):
    rows_local, cols_local, chans = inputs.shape
    grad_out, inputs = (jnp.swapaxes(grad_out, 1, 2), jnp.swapaxes(inputs, 1, 2))
    grad_out = pltpu.with_memory_space_constraint(grad_out, pltpu.HBM)
    inputs = pltpu.with_memory_space_constraint(inputs, pltpu.HBM)
    weight = pltpu.with_memory_space_constraint(weight, pltpu.HBM)
    half_rows, half_cols = rows_local // 2, cols_local // 2
    split = chans // 2
    chips = n_rows * n_cols // 2
    count = (27 + 1) // 2
    scale = 1.0 / math.sqrt(half_rows * n_rows * half_cols * n_cols)
    dma = pltpu.SemaphoreType.DMA
    vmem = pl.BlockSpec(memory_space=pltpu.VMEM)
    anywhere = pl.BlockSpec(memory_space=pl.ANY)
    hbm = pl.BlockSpec(memory_space=pltpu.HBM)
    input_grad, sums = pl.pallas_call(
        functools.partial(step_kernel, n_rows, n_cols, scale),
        out_shape=(
            jax.ShapeDtypeStruct(inputs.shape, BF16),
            jax.ShapeDtypeStruct((2 * count, split, LANES), BF16),
        ),
        in_specs=[hbm, hbm, hbm],
        out_specs=(vmem, vmem),
        scratch_shapes=[
            pltpu.VMEM(grad_out.shape, BF16),
            pltpu.VMEM(inputs.shape, BF16),
            pltpu.VMEM(weight.shape, BF16),
            pltpu.VMEM((chans, (half_rows + 1) * half_cols), BF16),
            pltpu.VMEM((half_rows + 1, EDGE, chans), BF16),
            pltpu.VMEM((chans, (half_rows + 1) * half_cols), BF16),
            pltpu.VMEM((EDGE, chans), BF16),
            pltpu.VMEM((2, 2, chans, half_rows * half_cols), BF16),
            pltpu.VMEM((2 * count, split, LANES), F32),
            pltpu.VMEM((count, split, LANES), F32),
            pltpu.VMEM((count, split, LANES), BF16),
            pltpu.VMEM((chips, split, LANES), BF16),
            pltpu.VMEM((2 * count, split, LANES), BF16),
            dma((3,)),
            dma((n_cols,)), dma((half_rows + 1,)), dma((n_cols,)), dma((half_rows + 1,)), dma((2, n_cols)),
            dma((count,)), dma((count,)),
            dma((PIECES, count)), dma((PIECES, chips)), dma((PIECES, chips)), dma((PIECES, count)),
            dma((PIECES, chips // n_cols, n_cols)), dma((PIECES, count)), dma((PIECES, count)),
        ],
        compiler_params=pltpu.CompilerParams(
            collective_id=0, has_side_effects=True, vmem_limit_bytes=48 * 1024 * 1024
        ),
    )(grad_out, inputs, weight)
    input_grad, filter_grad = pl.pallas_call(
        unpack_kernel,
        out_shape=(
            jax.ShapeDtypeStruct(inputs.shape, BF16),
            jax.ShapeDtypeStruct((9, chans, chans), F32),
        ),
        in_specs=[vmem, vmem],
        out_specs=(anywhere, anywhere),
        scratch_shapes=[pltpu.VMEM((9, chans, chans), F32), dma((10,))],
        compiler_params=pltpu.CompilerParams(vmem_limit_bytes=12 * 1024 * 1024),
    )(input_grad, sums)
    return jnp.swapaxes(input_grad, 1, 2), filter_grad.reshape(3, 3, chans, chans)


def solution(mesh):
    in_specs = (P(("rows", "cols"), None, None), P("rows", "cols", None), P())
    out_specs = (P("rows", "cols", None), P())
    return jax.shard_map(
        functools.partial(per_device, mesh.shape["rows"], mesh.shape["cols"]),
        mesh=mesh, in_specs=in_specs, out_specs=out_specs, check_vma=False,
    )
```
